32 devices in a mesh: gr: 8 (over z, x), gc: 4 (over y, core).
Axes of the slice: x: 2, y: 2, z: 4, core: 2. Of those that a mesh axis runs over, the one named last changes fastest.
Arguments:
- orbitals: bfloat16 [1536, 16384], P(None, ('gr', 'gc')), may hold values from -0.046875 to 0.046875
- velocities: bfloat16 [1536, 16384], P(None, ('gr', 'gc')), may hold values from -40 to 40
Outputs:
- new_velocities: float32 [1536, 16384], P(None, ('gr', 'gc'))
- violations: float32 [1], replicated
The draws below stay inside these ranges and needn't reach their ends.
All inputs are finite; a program needn't handle non-finite values.
Results may differ from the reference program's by a relative error of at most 0.0018.
Values may be sent and summed in bfloat16 or wider, within the bound.
No kernel may reach another device: no remote copies, remote signals or barrier semaphores. Data moves between devices by JAX's collectives and lax.ppermute only.
A program may use at most 64 MiB of HBM per device.

```python
import jax
import jax.numpy as jnp

M = 1536
ITERS = 1
GV = 16384


def draw_velocities(key, part):
    index = jnp.arange(M, dtype=jnp.float32)
    scale = jnp.exp(jnp.log(10.0) * index / (M - 1))
    base = jnp.clip(jax.random.normal(key, (M, GV), jnp.float32), -4.0, 4.0)
    return (base * scale[:, None]).astype(jnp.bfloat16)


def shard_levels(rng, extent, pieces, smallest, largest):
    loudness = 1.0
    for axis_at, shards_of in pieces:
        steps = jax.random.uniform(jax.random.fold_in(jax.random.fold_in(rng, 6), axis_at), (shards_of,), jnp.float32, smallest / len(pieces), largest / len(pieces))
        loudness = loudness * jnp.repeat(jnp.exp(steps), extent[axis_at] // shards_of).reshape((-1,) + (1,) * (len(extent) - 1 - axis_at))
    return loudness


def centred(rng, extent, scale, most, split=(), kind=jnp.bfloat16):
    entries = scale * jax.random.normal(rng, extent, jnp.float32)
    if split:
        entries = entries * shard_levels(rng, extent, split, -0.22, 0.18)
    return jnp.clip(entries, -most, most).astype(kind)


def setup_inputs(seed: int = 0) -> dict:
    splits = jax.random.split(jax.random.key(seed), 3)
    return {
        "orbitals": centred(splits[0], (M, GV), GV ** -0.5, 0.046875, ((1, 32),)),
        "velocities": draw_velocities(jax.random.fold_in(splits[2], 71), 0),
    }


def reference(orbitals, velocities):
    vel = velocities.astype(jnp.float32)
    measured = []
    for step in range(ITERS):
        vel_b = vel.astype(jnp.bfloat16)
        intersection = jnp.dot(orbitals, vel_b.T, preferred_element_type=jnp.float32)
        sym = intersection + intersection.T
        measured.append(jnp.sqrt(jnp.sum(sym * sym)) / M)
        sym_b = sym.astype(jnp.bfloat16)
        vel = vel - 0.5 * jnp.dot(sym_b, orbitals, preferred_element_type=jnp.float32)
    return (vel, jnp.stack(measured))
```

```python
import jax
import jax.numpy as jnp
from jax import lax
from jax.experimental import pallas as pl
from jax.experimental.pallas import tpu as pltpu
from jax.sharding import PartitionSpec as P

TILE = 128
CHUNKS = 2
PAD = 16
AXES = ("gr", "gc")
BF16 = jnp.bfloat16
F32 = jnp.float32
VMEM = pl.BlockSpec(memory_space=pltpu.VMEM)
SMEM = pl.BlockSpec(memory_space=pltpu.SMEM)


def layout(total_rows):
    tiles = total_rows // TILE
    side = tiles // 2
    extra = side // 2
    where = {}
    for i in range(side):
        for k in range(side):
            where[(i, i + k)] = i * side + k
    count = side * side + extra
    return side, extra, where, count


def product_kernel(half_ref, orb_ref, vel_ref, *out_refs, total_rows):
    side, extra, where, count = layout(total_rows)
    chunk_rows = count * TILE // CHUNKS
    h = half_ref[0]
    low = pl.multiple_of(h * (side * TILE), TILE)
    up = pl.multiple_of((1 - h) * (side * TILE), TILE)

    def put(index, value):
        value = value.astype(BF16)
        row = index * TILE
        end = row + TILE
        while row < end:
            chunk = row // chunk_rows
            stop = min(end, (chunk + 1) * chunk_rows)
            begin = index * TILE
            out_refs[chunk][row - chunk * chunk_rows : stop - chunk * chunk_rows, :] = value[
                row - begin : stop - begin
            ]
            row = stop

    def both(r0, rows, c0, cols):
        dims = (((1,), (1,)), ((), ()))
        one = lax.dot_general(
            orb_ref[pl.ds(r0, rows), :], vel_ref[pl.ds(c0, cols), :], dims, preferred_element_type=F32
        )
        two = lax.dot_general(
            vel_ref[pl.ds(r0, rows), :], orb_ref[pl.ds(c0, cols), :], dims, preferred_element_type=F32
        )
        return one + two

    for c in range(0, 2 * side - 1, 2):
        wide = min(2, 2 * side - 1 - c)
        first = max(0, c - side + 1)
        last = min(side - 1, c + wide - 1)
        start = low + c * TILE if c < side else up + (c - side) * TILE
        value = both(low + first * TILE, (last - first + 1) * TILE, start, wide * TILE)
        for i in range(first, last + 1):
            for k in range(wide):
                if (i, c + k) in where:
                    put(
                        where[(i, c + k)],
                        value[(i - first) * TILE : (i - first + 1) * TILE, k * TILE : (k + 1) * TILE],
                    )
    for k in range(extra):
        shift = pl.multiple_of((h * extra + k) * TILE, TILE)
        put(side * side + k, both(low + shift, TILE, up + shift, TILE))


def product(half, orb, vel):
    rows = orb.shape[0]
    count = layout(rows)[3]
    shape = jax.ShapeDtypeStruct((count * TILE // CHUNKS, TILE), BF16)
    return pl.pallas_call(
        lambda *refs: product_kernel(*refs, total_rows=rows),
        out_shape=[shape] * CHUNKS,
        in_specs=[SMEM, VMEM, VMEM],
        out_specs=[VMEM] * CHUNKS,
    )(half, orb, vel)


def share_kernel(off_ref, a_ref, b_ref, out_ref, *, side):
    rows = a_ref.shape[0]
    total = a_ref[...].astype(F32) + b_ref[...].astype(F32)
    out_ref[0:rows, :] = total.astype(BF16)
    row = lax.broadcasted_iota(jnp.int32, (rows, 1), 0) + off_ref[0]
    tile = row // TILE
    diagonal = (tile < side * side) & (tile % side == 0)
    weight = jnp.where(diagonal, 1.0, 2.0).astype(F32)
    square = jnp.sum(jnp.sum(total * total * weight, axis=0, keepdims=True), axis=1, keepdims=True)
    high = square.astype(BF16).astype(F32)
    rest = square - high
    middle = rest.astype(BF16).astype(F32)
    small = rest - middle
    line = lax.broadcasted_iota(jnp.int32, (PAD, TILE), 0)
    tail = jnp.where(line == 0, high, jnp.where(line == 1, middle, jnp.where(line == 2, small, 0.0)))
    out_ref[rows : rows + PAD, :] = tail.astype(BF16)


def make_share(offset, a, b, side):
    rows = a.shape[0]
    return pl.pallas_call(
        lambda *refs: share_kernel(*refs, side=side),
        out_shape=jax.ShapeDtypeStruct((rows + PAD, TILE), BF16),
        in_specs=[SMEM, VMEM, VMEM],
        out_specs=VMEM,
    )(offset, a, b)


def apply_kernel(half_ref, orb_ref, base_ref, *refs, total_rows, shares):
    side, extra, where, count = layout(total_rows)
    pieces = refs[:CHUNKS]
    out_ref, a_ref, b_ref, t_ref = refs[CHUNKS:]
    chunk_rows = count * TILE // CHUNKS
    share_rows = chunk_rows // shares
    h = half_ref[0]
    low = pl.multiple_of(h * (side * TILE), TILE)
    up = pl.multiple_of((1 - h) * (side * TILE), TILE)

    def tile(index):
        row, end = index * TILE, (index + 1) * TILE
        parts = []
        while row < end:
            chunk = row // chunk_rows
            inside = row - chunk * chunk_rows
            share = inside // share_rows
            stop = min(end, chunk * chunk_rows + (share + 1) * share_rows)
            at = share * (share_rows + PAD) + inside - share * share_rows
            parts.append(pieces[chunk][at : at + stop - row, :])
            row = stop
        return parts[0] if len(parts) == 1 else jnp.concatenate(parts, axis=0)

    zero = jnp.zeros((TILE, TILE), BF16)

    def block(ref, i, j, value):
        ref[i * TILE : (i + 1) * TILE, j * TILE : (j + 1) * TILE] = value

    for i in range(side):
        for j in range(i - i % 2, min(side, i - i % 2 + 2)):
            if j >= i:
                block(b_ref, i, j, zero)
                block(t_ref, j, i, zero)
    for (i, j), index in where.items():
        value = tile(index)
        if j < side:
            block(a_ref, i, j, value)
            if i != j:
                block(a_ref, j, i, value.T)
        else:
            block(b_ref, i, j - side, value)
            block(t_ref, j - side, i, value.T)
    for k in range(extra):
        value = tile(side * side + k)
        at = pl.multiple_of((h * extra + k) * TILE, TILE)
        b_ref[pl.ds(at, TILE), pl.ds(at, TILE)] = value
        t_ref[pl.ds(at, TILE), pl.ds(at, TILE)] = value.T

    wide = side * TILE
    panel = 2 * TILE
    for p in range(0, wide, panel):
        upto = min(p + panel, wide)
        rows = upto - p
        value = jnp.dot(a_ref[p:upto, :], orb_ref[pl.ds(low, wide), :], preferred_element_type=F32)
        value += jnp.dot(b_ref[p:upto, :upto], orb_ref[pl.ds(up, upto), :], preferred_element_type=F32)
        at = pl.ds(low + p, rows)
        out_ref[at, :] = base_ref[at, :].astype(F32) - 0.5 * value
        value = jnp.dot(
            t_ref[p:upto, p:], orb_ref[pl.ds(low + p, wide - p), :], preferred_element_type=F32
        )
        at = pl.ds(up + p, rows)
        out_ref[at, :] = base_ref[at, :].astype(F32) - 0.5 * value


def apply_half(half, orb, base, pieces, shares):
    rows = orb.shape[0]
    wide = layout(rows)[0] * TILE
    return pl.pallas_call(
        lambda *refs: apply_kernel(*refs, total_rows=rows, shares=shares),
        out_shape=jax.ShapeDtypeStruct(orb.shape, F32),
        in_specs=[SMEM] + [VMEM] * (2 + CHUNKS),
        out_specs=VMEM,
        scratch_shapes=[pltpu.VMEM((wide, wide), BF16)] * 3,
    )(half, orb, base, *pieces)


def pairs(nr, nc, even, odd):
    result = []
    for r in range(nr):
        for c in range(nc):
            flip = odd if c & 1 else even
            result.append((r * nc + c, (r ^ flip[0]) * nc + (c ^ flip[1])))
    return result


def local(orbitals, velocities):
    nr, nc = lax.axis_size("gr"), lax.axis_size("gc")
    r, c = lax.axis_index("gr"), lax.axis_index("gc")
    total_rows = orbitals.shape[0]
    side, _, _, count = layout(total_rows)
    core = c & 1
    on_r, on_c = r & 1, (c >> 1) & 1
    bit1 = jnp.where(core == 0, on_r, on_c)
    bit2 = jnp.where(core == 0, on_c, on_r)
    swap = pairs(nr, nc, (0, 1), (0, 1))
    first = pairs(nr, nc, (1, 0), (0, 2))
    second = pairs(nr, nc, (0, 2), (1, 0))
    rest = [(1 << b, 0) for b in range(1, nr.bit_length() - 1)]
    rest += [(0, 1 << b) for b in range(2, nc.bit_length() - 1)]
    doubling = [pairs(nr, nc, rest[k], rest[-1 - k]) for k in range(len(rest))]
    shares = 4
    chunk_rows = count * TILE // CHUNKS
    half_rows, share_rows = chunk_rows // 2, chunk_rows // 4

    def move(value, perm):
        return lax.ppermute(value, AXES, perm)

    def cut(value, index, rows):
        return lax.dynamic_slice_in_dim(value, index * rows, rows, 0).astype(F32)

    def rounded(value):
        return lax.reduce_precision(value, 8, 7)

    own = core.reshape(1)
    other = (1 - core).reshape(1)
    away = product(other, orbitals, velocities)
    away = [move(x, swap) for x in away]
    keep = product(own, orbitals, velocities)
    joined = []
    for k in range(CHUNKS):
        mine, got = keep[k], away[k]
        send = cut(mine, 1 - bit1, half_rows) + cut(got, 1 - bit1, half_rows)
        got1 = move(send.astype(BF16), first)
        mine1 = cut(mine, bit1, half_rows) + cut(got, bit1, half_rows)
        send = cut(mine1, 1 - bit2, share_rows) + cut(got1, 1 - bit2, share_rows)
        got2 = move(send.astype(BF16), second)
        mine2 = cut(mine1, bit2, share_rows) + cut(got1, bit2, share_rows)
        total = rounded(mine2 + got2.astype(F32))
        for j, perm in enumerate(doubling):
            sent = total.astype(BF16)
            back = move(sent, perm)
            if j < len(doubling) - 1:
                total = rounded(total + back.astype(F32))
        offset = k * chunk_rows + bit1 * half_rows + bit2 * share_rows
        share = make_share(offset.reshape(1), sent, back, side)
        back = move(share, second)
        low = jnp.where(bit2 == 0, share, back)
        high = jnp.where(bit2 == 0, back, share)
        quarter = jnp.concatenate([low, high], axis=0)
        back = move(quarter, first)
        low = jnp.where(bit1 == 0, quarter, back)
        high = jnp.where(bit1 == 0, back, quarter)
        joined.append(jnp.concatenate([low, high], axis=0))
    far = [move(x, swap) for x in joined]
    partial = apply_half(own, orbitals, velocities, joined, shares)
    new = apply_half(other, orbitals, partial, far, shares)

    def squares(pieces):
        total = 0.0
        for x in pieces:
            tails = x.reshape(shares, share_rows + PAD, TILE)[:, share_rows : share_rows + 3, 0]
            total = total + jnp.sum(tails.astype(F32))
        return total

    measured = jnp.sqrt(squares(joined) + squares(far)) / total_rows
    return new, measured.reshape(1)


def solution(mesh):
    in_specs = (P(None, AXES), P(None, AXES))
    out_specs = (P(None, AXES), P())
    return jax.shard_map(local, mesh=mesh, in_specs=in_specs, out_specs=out_specs, check_vma=False)
```

```python
import jax
import jax.numpy as jnp
from jax import lax
from jax.experimental import pallas as pl
from jax.experimental.pallas import tpu as pltpu
from jax.sharding import PartitionSpec as P


TILE = 128
PAD = 16
SHARES = 4
AXES = ("gr", "gc")
BF16 = jnp.bfloat16
F32 = jnp.float32
VMEM = pl.BlockSpec(memory_space=pltpu.VMEM)
SMEM = pl.BlockSpec(memory_space=pltpu.SMEM)
DIMS = (((1,), (1,)), ((), ()))


def params(mib):
    return pltpu.CompilerParams(vmem_limit_bytes=mib * 2**20)


def layout(total_rows):
    side = total_rows // TILE // 2
    extra = side // 2
    near = [(i, j) for i in range(side) for j in range(i, side)]
    far = [(i, j) for i in range(side) for j in range(i)]
    near_at = {ij: n for n, ij in enumerate(near)}
    far_at = {ij: n for n, ij in enumerate(far)}
    return side, extra, near_at, far_at


def starts(half_ref, side):
    h = half_ref[0]
    low = pl.multiple_of(h * (side * TILE), TILE)
    up = pl.multiple_of((1 - h) * (side * TILE), TILE)
    return h, low, up


def symmetric(orb_ref, vel_ref, r0, rows, c0, cols):
    one = lax.dot_general(
        orb_ref[pl.ds(r0, rows), :], vel_ref[pl.ds(c0, cols), :], DIMS, preferred_element_type=F32
    )
    two = lax.dot_general(
        vel_ref[pl.ds(r0, rows), :], orb_ref[pl.ds(c0, cols), :], DIMS, preferred_element_type=F32
    )
    return one + two


def product_kernel(half_ref, orb_ref, vel_ref, out_ref, *, chunk, total_rows):
    side, extra, near_at, far_at = layout(total_rows)
    h, low, up = starts(half_ref, side)
    table = far_at if chunk else near_at
    for c in range(0, side, 2):
        columns = [j for j in (c, c + 1) if j < side]
        rows = [i for i in range(side) if any((i, j) in table for j in columns)]
        columns = [j for j in columns if any((i, j) in table for i in rows)]
        if not rows:
            continue
        value = symmetric(
            orb_ref,
            vel_ref,
            low + rows[0] * TILE,
            len(rows) * TILE,
            (up if chunk else low) + columns[0] * TILE,
            len(columns) * TILE,
        )
        for i in rows:
            for j in columns:
                if (i, j) in table:
                    at = table[(i, j)] * TILE
                    row, col = (i - rows[0]) * TILE, (j - columns[0]) * TILE
                    out_ref[at : at + TILE, :] = value[row : row + TILE, col : col + TILE].astype(BF16)
    if chunk:
        for k in range(extra):
            shift = pl.multiple_of((h * extra + k) * TILE, TILE)
            at = (len(far_at) + k) * TILE
            value = symmetric(orb_ref, vel_ref, low + shift, TILE, up + shift, TILE)
            out_ref[at : at + TILE, :] = value.astype(BF16)


def tile_count(chunk, total_rows):
    _, extra, near_at, far_at = layout(total_rows)
    return len(far_at) + extra if chunk else len(near_at)


def product(half, orb, vel, chunk):
    rows = orb.shape[0]
    return pl.pallas_call(
        lambda *refs: product_kernel(*refs, chunk=chunk, total_rows=rows),
        out_shape=jax.ShapeDtypeStruct((tile_count(chunk, rows) * TILE, TILE), BF16),
        in_specs=[SMEM, VMEM, VMEM],
        out_specs=VMEM,
        compiler_params=params(16),
    )(half, orb, vel)


def share_kernel(off_ref, a_ref, b_ref, out_ref, *, diagonal):
    rows = a_ref.shape[0]
    total = a_ref[...].astype(F32) + b_ref[...].astype(F32)
    out_ref[0:rows, :] = total.astype(BF16)
    square = total * total
    if diagonal:
        tile = (lax.broadcasted_iota(jnp.int32, (rows, TILE), 0) + off_ref[0]) // TILE
        single = tile == diagonal[0]
        for at in diagonal[1:]:
            single |= tile == at
        square = jnp.where(single, square, 2.0 * square)
    else:
        square = 2.0 * square
    square = jnp.sum(jnp.sum(square, axis=0, keepdims=True), axis=1, keepdims=True)
    high = square.astype(BF16).astype(F32)
    rest = square - high
    middle = rest.astype(BF16).astype(F32)
    small = rest - middle
    line = lax.broadcasted_iota(jnp.int32, (PAD, TILE), 0)
    tail = jnp.where(line == 0, high, jnp.where(line == 1, middle, jnp.where(line == 2, small, 0.0)))
    out_ref[rows : rows + PAD, :] = tail.astype(BF16)


def make_share(offset, a, b, diagonal):
    rows = a.shape[0]
    return pl.pallas_call(
        lambda *refs: share_kernel(*refs, diagonal=diagonal),
        out_shape=jax.ShapeDtypeStruct((rows + PAD, TILE), BF16),
        in_specs=[SMEM, VMEM, VMEM],
        out_specs=VMEM,
        compiler_params=params(4),
    )(offset, a, b)


def take_tile(ref, index):
    share_rows = ref.shape[0] // SHARES - PAD
    row, end = index * TILE, (index + 1) * TILE
    parts = []
    while row < end:
        share = row // share_rows
        stop = min(end, (share + 1) * share_rows)
        parts.append(ref[row + share * PAD : stop + share * PAD, :])
        row = stop
    return parts[0] if len(parts) == 1 else jnp.concatenate(parts, axis=0)


def put_block(ref, i, j, value):
    ref[i * TILE : (i + 1) * TILE, j * TILE : (j + 1) * TILE] = value


def near_kernel(half_ref, orb_ref, vel_ref, own_ref, far_ref, out_ref, a_ref):
    side, _, near_at, _ = layout(orb_ref.shape[0])
    wide = side * TILE
    _, low, up = starts(half_ref, side)
    for ref, at, n in ((own_ref, low, 0), (far_ref, up, 1)):
        for (i, j), index in near_at.items():
            value = take_tile(ref, index)
            put_block(a_ref, i + n * side, j, value)
            if i != j:
                put_block(a_ref, j + n * side, i, value.T)
        value = jnp.dot(
            a_ref[n * wide : (n + 1) * wide, :], orb_ref[pl.ds(at, wide), :], preferred_element_type=F32
        )
        out_ref[pl.ds(at, wide), :] = vel_ref[pl.ds(at, wide), :].astype(F32) - 0.5 * value


def apply_near(half, orb, vel, own, far):
    wide = orb.shape[0] // 2
    return pl.pallas_call(
        near_kernel,
        out_shape=jax.ShapeDtypeStruct(orb.shape, F32),
        in_specs=[SMEM] + [VMEM] * 4,
        out_specs=VMEM,
        scratch_shapes=[pltpu.VMEM((2 * wide, wide), BF16)],
        compiler_params=params(20),
    )(half, orb, vel, own, far)


def tails(ref):
    share = ref.shape[0] // SHARES
    total = jnp.zeros((1, TILE), F32)
    for k in range(SHARES):
        lines = ref[(k + 1) * share - PAD : (k + 1) * share, :].astype(F32)
        total = total + jnp.sum(lines, axis=0, keepdims=True)
    return total


def far_kernel(half_ref, orb_ref, base_ref, piece_ref, *refs):
    total_rows = orb_ref.shape[0]
    side, extra, _, far_at = layout(total_rows)
    h, low, up = starts(half_ref, side)
    out_ref, b_ref, t_ref = refs[-3:]
    if len(refs) > 3:
        near_own, near_far, own, out_ref, norm_ref = refs[:5]
        square = (tails(near_own) + tails(own)) + (tails(near_far) + tails(piece_ref))
        norm_ref[0] = (jnp.sqrt(square) / total_rows)[0, 0]
    zero = jnp.zeros((TILE, TILE), BF16)
    for i in range(side):
        for j in range(i, i - i % 2 + 2):
            if j < side:
                put_block(b_ref, i, j, zero)
                put_block(t_ref, j, i, zero)
    for (i, j), index in far_at.items():
        value = take_tile(piece_ref, index)
        put_block(b_ref, i, j, value)
        put_block(t_ref, j, i, value.T)
    for k in range(extra):
        value = take_tile(piece_ref, len(far_at) + k)
        at = pl.multiple_of((h * extra + k) * TILE, TILE)
        b_ref[pl.ds(at, TILE), pl.ds(at, TILE)] = value
        t_ref[pl.ds(at, TILE), pl.ds(at, TILE)] = value.T
    wide = side * TILE
    panel = 2 * TILE
    for p in range(0, wide, panel):
        end = min(p + panel, wide)
        value = jnp.dot(b_ref[p:end, :end], orb_ref[pl.ds(up, end), :], preferred_element_type=F32)
        at = pl.ds(low + p, end - p)
        out_ref[at, :] = base_ref[at, :] - 0.5 * value
        value = jnp.dot(t_ref[p:end, p:], orb_ref[pl.ds(low + p, wide - p), :], preferred_element_type=F32)
        at = pl.ds(up + p, end - p)
        out_ref[at, :] = base_ref[at, :] - 0.5 * value


def apply_far(half, orb, base, piece, others=()):
    wide = orb.shape[0] // 2
    out_shape = [jax.ShapeDtypeStruct(orb.shape, F32)]
    out_specs = [VMEM]
    if others:
        out_shape.append(jax.ShapeDtypeStruct((1,), F32))
        out_specs.append(SMEM)
    return pl.pallas_call(
        far_kernel,
        out_shape=out_shape,
        in_specs=[SMEM] + [VMEM] * (3 + len(others)),
        out_specs=out_specs,
        scratch_shapes=[pltpu.VMEM((wide, wide), BF16)] * 2,
        compiler_params=params(20),
    )(half, orb, base, piece, *others)


def pairs(nr, nc, even, odd):
    result = []
    for r in range(nr):
        for c in range(nc):
            flip = odd if c & 1 else even
            result.append((r * nc + c, (r ^ flip[0]) * nc + (c ^ flip[1])))
    return result


def local(orbitals, velocities):
    nr, nc = lax.axis_size("gr"), lax.axis_size("gc")
    r, c = lax.axis_index("gr"), lax.axis_index("gc")
    side, _, near_at, _ = layout(orbitals.shape[0])
    core = c & 1
    on_r, on_c = r & 1, (c >> 1) & 1
    bit1 = jnp.where(core == 0, on_r, on_c)
    bit2 = jnp.where(core == 0, on_c, on_r)
    swap = pairs(nr, nc, (0, 1), (0, 1))
    first = pairs(nr, nc, (1, 0), (0, 2))
    second = pairs(nr, nc, (0, 2), (1, 0))
    rest = [(1 << b, 0) for b in range(1, nr.bit_length() - 1)]
    rest += [(0, 1 << b) for b in range(2, nc.bit_length() - 1)]
    doubling = [pairs(nr, nc, rest[k], rest[-1 - k]) for k in range(len(rest))]
    diagonals = [[near_at[(i, i)] for i in range(side)], []]

    def move(value, perm):
        return lax.ppermute(value, AXES, perm)

    def cut(value, index, rows):
        return lax.dynamic_slice_in_dim(value, index * rows, rows, 0).astype(F32)

    def rounded(value):
        return lax.reduce_precision(value, 8, 7)

    def join(bit, mine, got):
        return jnp.concatenate([jnp.where(bit == 0, mine, got), jnp.where(bit == 0, got, mine)], axis=0)

    own = core.reshape(1)
    other = (1 - core).reshape(1)
    joined = []
    for k in range(2):
        away = product(other, orbitals, velocities, k)
        got = move(away, swap)
        mine = product(own, orbitals, velocities, k)
        rows = mine.shape[0]
        half, quarter = rows // 2, rows // 4
        send = (cut(mine, 1 - bit1, half) + cut(got, 1 - bit1, half)).astype(BF16)
        mine1 = cut(mine, bit1, half) + cut(got, bit1, half)
        got1 = move(send, first)
        send = (cut(mine1, 1 - bit2, quarter) + cut(got1, 1 - bit2, quarter)).astype(BF16)
        mine2 = cut(mine1, bit2, quarter) + cut(got1, bit2, quarter)
        got2 = move(send, second)
        total = rounded(mine2 + got2.astype(F32))
        for j, perm in enumerate(doubling):
            sent = total.astype(BF16)
            back = move(sent, perm)
            if j < len(doubling) - 1:
                total = rounded(total + back.astype(F32))
        share = make_share((bit1 * half + bit2 * quarter).reshape(1), sent, back, diagonals[k])
        back = move(share, second)
        quarter = join(bit2, share, back)
        back = move(quarter, first)
        joined.append(join(bit1, quarter, back))
    far = [move(joined[k], swap) for k in range(2)]
    new = apply_near(own, orbitals, velocities, joined[0], far[0])
    (new,) = apply_far(own, orbitals, new, joined[1])
    new, measured = apply_far(other, orbitals, new, far[1], (joined[0], far[0], joined[1]))
    return new, measured


def solution(mesh):
    in_specs = (P(None, AXES), P(None, AXES))
    out_specs = (P(None, AXES), P())

    return jax.shard_map(local, mesh=mesh, in_specs=in_specs, out_specs=out_specs, check_vma=False)
```

```python
import jax
import jax.numpy as jnp
from jax import lax
from jax.experimental import pallas as pl
from jax.experimental.pallas import tpu as pltpu
from jax.sharding import PartitionSpec as P


TILE = 128
PAD = 16
SHARES = 4
AXES = ("gr", "gc")
BF16 = jnp.bfloat16
F32 = jnp.float32
VMEM = pl.BlockSpec(memory_space=pltpu.VMEM)
SMEM = pl.BlockSpec(memory_space=pltpu.SMEM)
DIMS = (((1,), (1,)), ((), ()))


def params(mib):
    return pltpu.CompilerParams(vmem_limit_bytes=mib * 2**20)


def layout(total_rows):
    side = total_rows // TILE // 2
    extra = side // 2
    near = [(i, j) for i in range(side) for j in range(i, side)]
    far = [(i, j) for i in range(side) for j in range(i)]
    near_at = {ij: n for n, ij in enumerate(near)}
    far_at = {ij: n for n, ij in enumerate(far)}
    return side, extra, near_at, far_at


def position():
    r, c = lax.axis_index("gr"), lax.axis_index("gc")
    core = c & 1
    on_r, on_c = r & 1, (c >> 1) & 1
    return core, jnp.where(core == 0, on_r, on_c), jnp.where(core == 0, on_c, on_r)


def starts(flip, side):
    core, _, _ = position()
    h = core ^ flip
    low = pl.multiple_of(h * (side * TILE), TILE)
    up = pl.multiple_of((1 - h) * (side * TILE), TILE)
    return h, low, up


def symmetric(orb_ref, vel_ref, r0, rows, c0, cols):
    one = lax.dot_general(
        orb_ref[pl.ds(r0, rows), :], vel_ref[pl.ds(c0, cols), :], DIMS, preferred_element_type=F32
    )
    two = lax.dot_general(
        vel_ref[pl.ds(r0, rows), :], orb_ref[pl.ds(c0, cols), :], DIMS, preferred_element_type=F32
    )
    return one + two


def product_kernel(orb_ref, vel_ref, out_ref, *, flip, chunk, total_rows):
    side, extra, near_at, far_at = layout(total_rows)
    h, low, up = starts(flip, side)
    table = far_at if chunk else near_at
    for c in range(0, side, 2):
        columns = [j for j in (c, c + 1) if j < side]
        rows = [i for i in range(side) if any((i, j) in table for j in columns)]
        columns = [j for j in columns if any((i, j) in table for i in rows)]
        if not rows:
            continue
        value = symmetric(
            orb_ref,
            vel_ref,
            low + rows[0] * TILE,
            len(rows) * TILE,
            (up if chunk else low) + columns[0] * TILE,
            len(columns) * TILE,
        )
        for i in rows:
            for j in columns:
                if (i, j) in table:
                    at = table[(i, j)] * TILE
                    row, col = (i - rows[0]) * TILE, (j - columns[0]) * TILE
                    out_ref[at : at + TILE, :] = value[row : row + TILE, col : col + TILE].astype(BF16)
    if chunk:
        for k in range(extra):
            shift = pl.multiple_of((h * extra + k) * TILE, TILE)
            at = (len(far_at) + k) * TILE
            value = symmetric(orb_ref, vel_ref, low + shift, TILE, up + shift, TILE)
            out_ref[at : at + TILE, :] = value.astype(BF16)


def tile_count(chunk, total_rows):
    _, extra, near_at, far_at = layout(total_rows)
    return len(far_at) + extra if chunk else len(near_at)


def call(kernel, out, mib, *operands, scratch=()):
    return pl.pallas_call(
        kernel,
        out_shape=out,
        in_specs=[VMEM] * len(operands),
        out_specs=jax.tree.map(lambda _: VMEM, out),
        scratch_shapes=scratch,
        compiler_params=params(mib),
    )(*operands)


def product(flip, orb, vel, chunk):
    rows = orb.shape[0]
    return call(
        lambda *refs: product_kernel(*refs, flip=flip, chunk=chunk, total_rows=rows),
        jax.ShapeDtypeStruct((tile_count(chunk, rows) * TILE, TILE), BF16),
        6,
        orb,
        vel,
    )


def halve_kernel(mine_ref, got_ref, send_ref, keep_ref, *, which):
    rows = send_ref.shape[0]
    bit = position()[which]

    def part(index):
        at = pl.ds(pl.multiple_of(index * rows, PAD), rows)
        return mine_ref[at, :].astype(F32) + got_ref[at, :].astype(F32)

    send_ref[...] = part(1 - bit).astype(BF16)
    keep_ref[...] = part(bit)


def halve(mine, got, which):
    rows = mine.shape[0] // 2
    out = [jax.ShapeDtypeStruct((rows, TILE), BF16), jax.ShapeDtypeStruct((rows, TILE), F32)]
    return call(lambda *refs: halve_kernel(*refs, which=which), out, 2, mine, got)


def add_kernel(a_ref, b_ref, out_ref):
    out_ref[...] = (a_ref[...].astype(F32) + b_ref[...].astype(F32)).astype(BF16)


def add(a, b):
    return call(add_kernel, jax.ShapeDtypeStruct(a.shape, BF16), 2, a, b)


def join_kernel(mine_ref, got_ref, out_ref, *, which):
    rows = mine_ref.shape[0]
    bit = position()[which]
    out_ref[pl.ds(pl.multiple_of(bit * rows, PAD), rows), :] = mine_ref[...]
    out_ref[pl.ds(pl.multiple_of((1 - bit) * rows, PAD), rows), :] = got_ref[...]


def join(mine, got, which):
    out = jax.ShapeDtypeStruct((2 * mine.shape[0], TILE), BF16)
    return call(lambda *refs: join_kernel(*refs, which=which), out, 2, mine, got)


def share_kernel(a_ref, b_ref, out_ref, *, diagonal):
    rows = a_ref.shape[0]
    _, bit1, bit2 = position()
    offset = (2 * bit1 + bit2) * rows
    total = a_ref[...].astype(F32) + b_ref[...].astype(F32)
    out_ref[0:rows, :] = total.astype(BF16)
    square = total * total
    if diagonal:
        tile = (lax.broadcasted_iota(jnp.int32, (rows, TILE), 0) + offset) // TILE
        single = tile == diagonal[0]
        for at in diagonal[1:]:
            single |= tile == at
        square = jnp.where(single, square, 2.0 * square)
    else:
        square = 2.0 * square
    square = jnp.sum(jnp.sum(square, axis=0, keepdims=True), axis=1, keepdims=True)
    high = square.astype(BF16).astype(F32)
    rest = square - high
    middle = rest.astype(BF16).astype(F32)
    small = rest - middle
    line = lax.broadcasted_iota(jnp.int32, (PAD, TILE), 0)
    tail = jnp.where(line == 0, high, jnp.where(line == 1, middle, jnp.where(line == 2, small, 0.0)))
    out_ref[rows : rows + PAD, :] = tail.astype(BF16)


def make_share(a, b, diagonal):
    out = jax.ShapeDtypeStruct((a.shape[0] + PAD, TILE), BF16)
    return call(lambda *refs: share_kernel(*refs, diagonal=diagonal), out, 3, a, b)


def take_tile(ref, index):
    share_rows = ref.shape[0] // SHARES - PAD
    row, end = index * TILE, (index + 1) * TILE
    parts = []
    while row < end:
        share = row // share_rows
        stop = min(end, (share + 1) * share_rows)
        parts.append(ref[row + share * PAD : stop + share * PAD, :])
        row = stop
    return parts[0] if len(parts) == 1 else jnp.concatenate(parts, axis=0)


def put_block(ref, i, j, value):
    ref[i * TILE : (i + 1) * TILE, j * TILE : (j + 1) * TILE] = value


def near_kernel(orb_ref, vel_ref, own_ref, far_ref, out_ref, a_ref):
    side, _, near_at, _ = layout(orb_ref.shape[0])
    wide = side * TILE
    _, low, up = starts(0, side)
    for ref, at, n in ((own_ref, low, 0), (far_ref, up, 1)):
        for (i, j), index in near_at.items():
            value = take_tile(ref, index)
            put_block(a_ref, i + n * side, j, value)
            if i != j:
                put_block(a_ref, j + n * side, i, value.T)
        value = jnp.dot(
            a_ref[n * wide : (n + 1) * wide, :], orb_ref[pl.ds(at, wide), :], preferred_element_type=F32
        )
        out_ref[pl.ds(at, wide), :] = vel_ref[pl.ds(at, wide), :].astype(F32) - 0.5 * value


def apply_near(orb, vel, own, far):
    wide = orb.shape[0] // 2
    out = jax.ShapeDtypeStruct(orb.shape, F32)
    return call(near_kernel, out, 8, orb, vel, own, far, scratch=[pltpu.VMEM((2 * wide, wide), BF16)])


def tails(ref):
    share = ref.shape[0] // SHARES
    total = jnp.zeros((1, TILE), F32)
    for k in range(SHARES):
        lines = ref[(k + 1) * share - PAD : (k + 1) * share, :].astype(F32)
        total = total + jnp.sum(lines, axis=0, keepdims=True)
    return total


def far_kernel(orb_ref, base_ref, piece_ref, *refs, flip):
    total_rows = orb_ref.shape[0]
    side, extra, _, far_at = layout(total_rows)
    h, low, up = starts(flip, side)
    out_ref, b_ref, t_ref = refs[-3:]
    if len(refs) > 3:
        near_own, near_far, own, out_ref, norm_ref = refs[:5]
        square = (tails(near_own) + tails(own)) + (tails(near_far) + tails(piece_ref))
        norm_ref[0] = (jnp.sqrt(square) / total_rows)[0, 0]
    zero = jnp.zeros((TILE, TILE), BF16)
    for i in range(side):
        for j in range(i, i - i % 2 + 2):
            if j < side:
                put_block(b_ref, i, j, zero)
                put_block(t_ref, j, i, zero)
    for (i, j), index in far_at.items():
        value = take_tile(piece_ref, index)
        put_block(b_ref, i, j, value)
        put_block(t_ref, j, i, value.T)
    for k in range(extra):
        value = take_tile(piece_ref, len(far_at) + k)
        at = pl.multiple_of((h * extra + k) * TILE, TILE)
        b_ref[pl.ds(at, TILE), pl.ds(at, TILE)] = value
        t_ref[pl.ds(at, TILE), pl.ds(at, TILE)] = value.T
    wide = side * TILE
    panel = 2 * TILE
    for p in range(0, wide, panel):
        end = min(p + panel, wide)
        value = jnp.dot(b_ref[p:end, :end], orb_ref[pl.ds(up, end), :], preferred_element_type=F32)
        at = pl.ds(low + p, end - p)
        out_ref[at, :] = base_ref[at, :] - 0.5 * value
        value = jnp.dot(t_ref[p:end, p:], orb_ref[pl.ds(low + p, wide - p), :], preferred_element_type=F32)
        at = pl.ds(up + p, end - p)
        out_ref[at, :] = base_ref[at, :] - 0.5 * value


def apply_far(flip, orb, base, piece, others=()):
    wide = orb.shape[0] // 2
    out_shape = [jax.ShapeDtypeStruct(orb.shape, F32)]
    out_specs = [VMEM]
    if others:
        out_shape.append(jax.ShapeDtypeStruct((1,), F32))
        out_specs.append(SMEM)
    return pl.pallas_call(
        lambda *refs: far_kernel(*refs, flip=flip),
        out_shape=out_shape,
        in_specs=[VMEM] * (3 + len(others)),
        out_specs=out_specs,
        scratch_shapes=[pltpu.VMEM((wide, wide), BF16)] * 2,
        compiler_params=params(8),
    )(orb, base, piece, *others)


def pairs(nr, nc, even, odd):
    result = []
    for r in range(nr):
        for c in range(nc):
            flip = odd if c & 1 else even
            result.append((r * nc + c, (r ^ flip[0]) * nc + (c ^ flip[1])))
    return result


def local(orbitals, velocities):
    nr, nc = lax.axis_size("gr"), lax.axis_size("gc")
    side, _, near_at, _ = layout(orbitals.shape[0])
    swap = pairs(nr, nc, (0, 1), (0, 1))
    first = pairs(nr, nc, (1, 0), (0, 2))
    second = pairs(nr, nc, (0, 2), (1, 0))
    rest = [(1 << b, 0) for b in range(1, nr.bit_length() - 1)]
    rest += [(0, 1 << b) for b in range(2, nc.bit_length() - 1)]
    doubling = [pairs(nr, nc, rest[k], rest[-1 - k]) for k in range(len(rest))]
    diagonals = [[near_at[(i, i)] for i in range(side)], []]

    def move(value, perm):
        return lax.ppermute(value, AXES, perm)

    joined = []
    for k in range(2):
        away = product(1, orbitals, velocities, k)
        got = move(away, swap)
        mine = product(0, orbitals, velocities, k)
        send, mine = halve(mine, got, 1)
        got = move(send, first)
        send, mine = halve(mine, got, 2)
        got = move(send, second)
        for perm in doubling:
            mine = add(mine, got)
            got = move(mine, perm)
        share = make_share(mine, got, diagonals[k])
        got = move(share, second)
        quarter = join(share, got, 2)
        got = move(quarter, first)
        joined.append(join(quarter, got, 1))
    far = [move(joined[k], swap) for k in range(2)]
    new = apply_near(orbitals, velocities, joined[0], far[0])
    (new,) = apply_far(0, orbitals, new, joined[1])
    new, measured = apply_far(1, orbitals, new, far[1], (joined[0], far[0], joined[1]))
    return new, measured


def solution(mesh):
    in_specs = (P(None, AXES), P(None, AXES))
    out_specs = (P(None, AXES), P())

    return jax.shard_map(local, mesh=mesh, in_specs=in_specs, out_specs=out_specs, check_vma=False)
```

```python
import jax
import jax.numpy as jnp
from jax import lax
from jax.experimental import pallas as pl
from jax.experimental.pallas import tpu as pltpu
from jax.sharding import PartitionSpec as P


TILE = 128
PAD = 16
SHARES = 4
AXES = ("gr", "gc")
BF16 = jnp.bfloat16
F32 = jnp.float32
VMEM = pl.BlockSpec(memory_space=pltpu.VMEM)
SMEM = pl.BlockSpec(memory_space=pltpu.SMEM)
DIMS = (((1,), (1,)), ((), ()))


def params(mib):
    return pltpu.CompilerParams(vmem_limit_bytes=mib * 2**20)


def layout(total_rows):
    side = total_rows // TILE // 2
    extra = side // 2
    near = [(i, j) for i in range(side) for j in range(i, side)]
    far = [(i, j) for i in range(side) for j in range(i)]
    near_at = {ij: n for n, ij in enumerate(near)}
    far_at = {ij: n for n, ij in enumerate(far)}
    return side, extra, near_at, far_at


def parity(r, c):
    return (r ^ (r >> 1) ^ (c >> 1)) & 1


def position():
    r, c = lax.axis_index("gr"), lax.axis_index("gc")
    half = (c & 1) ^ parity(r, c)
    on_r, on_c = r & 1, (c >> 1) & 1
    return half, jnp.where(half == 0, on_r, on_c), jnp.where(half == 0, on_c, on_r)


def starts(flip, side):
    half, _, _ = position()
    h = half ^ flip
    low = pl.multiple_of(h * (side * TILE), TILE)
    up = pl.multiple_of((1 - h) * (side * TILE), TILE)
    return h, low, up


def symmetric(orb_ref, vel_ref, r0, rows, c0, cols):
    one = lax.dot_general(
        orb_ref[pl.ds(r0, rows), :], vel_ref[pl.ds(c0, cols), :], DIMS, preferred_element_type=F32
    )
    two = lax.dot_general(
        vel_ref[pl.ds(r0, rows), :], orb_ref[pl.ds(c0, cols), :], DIMS, preferred_element_type=F32
    )
    return one + two


def product_kernel(orb_ref, vel_ref, out_ref, *, flip, chunk, total_rows):
    side, extra, near_at, far_at = layout(total_rows)
    h, low, up = starts(flip, side)
    table = far_at if chunk else near_at
    for c in range(0, side, 2):
        columns = [j for j in (c, c + 1) if j < side]
        rows = [i for i in range(side) if any((i, j) in table for j in columns)]
        columns = [j for j in columns if any((i, j) in table for i in rows)]
        if not rows:
            continue
        value = symmetric(
            orb_ref,
            vel_ref,
            low + rows[0] * TILE,
            len(rows) * TILE,
            (up if chunk else low) + columns[0] * TILE,
            len(columns) * TILE,
        )
        for i in rows:
            for j in columns:
                if (i, j) in table:
                    at = table[(i, j)] * TILE
                    row, col = (i - rows[0]) * TILE, (j - columns[0]) * TILE
                    out_ref[at : at + TILE, :] = value[row : row + TILE, col : col + TILE].astype(BF16)
    if chunk:
        for k in range(extra):
            shift = pl.multiple_of((h * extra + k) * TILE, TILE)
            at = (len(far_at) + k) * TILE
            value = symmetric(orb_ref, vel_ref, low + shift, TILE, up + shift, TILE)
            out_ref[at : at + TILE, :] = value.astype(BF16)


def tile_count(chunk, total_rows):
    _, extra, near_at, far_at = layout(total_rows)
    return len(far_at) + extra if chunk else len(near_at)


def call(kernel, out, mib, *operands, scratch=()):
    return pl.pallas_call(
        kernel,
        out_shape=out,
        in_specs=[VMEM] * len(operands),
        out_specs=jax.tree.map(lambda _: VMEM, out),
        scratch_shapes=scratch,
        compiler_params=params(mib),
    )(*operands)


def load_kernel(orb_hbm, vel_hbm, away_ref, orb_ref, vel_ref, sems):
    total_rows = orb_hbm.shape[0]
    _, low, up = starts(1, layout(total_rows)[0])
    rows = total_rows // 4
    copies = []
    for at in (low, low + rows, up, up + rows):
        for source, target in ((orb_hbm, orb_ref), (vel_hbm, vel_ref)):
            part = pl.ds(pl.multiple_of(at, TILE), rows)
            copies.append(pltpu.make_async_copy(source.at[part], target.at[part], sems.at[len(copies)]))
            copies[-1].start()
    for copy in copies[:4]:
        copy.wait()
    product_kernel(orb_ref, vel_ref, away_ref, flip=1, chunk=0, total_rows=total_rows)
    for copy in copies[4:]:
        copy.wait()


def load(orb, vel):
    rows = orb.shape[0]
    whole = jax.ShapeDtypeStruct(orb.shape, orb.dtype)
    return pl.pallas_call(
        load_kernel,
        out_shape=[jax.ShapeDtypeStruct((tile_count(0, rows) * TILE, TILE), BF16), whole, whole],
        in_specs=[pl.BlockSpec(memory_space=pltpu.HBM)] * 2,
        out_specs=[VMEM] * 3,
        scratch_shapes=[pltpu.SemaphoreType.DMA((8,))],
        compiler_params=params(12),
    )(orb, vel)


def product(flip, orb, vel, chunk):
    rows = orb.shape[0]
    return call(
        lambda *refs: product_kernel(*refs, flip=flip, chunk=chunk, total_rows=rows),
        jax.ShapeDtypeStruct((tile_count(chunk, rows) * TILE, TILE), BF16),
        6,
        orb,
        vel,
    )


def halve_kernel(mine_ref, got_ref, send_ref, keep_ref, *, which):
    rows = send_ref.shape[0]
    bit = position()[which]

    def part(index):
        at = pl.ds(pl.multiple_of(index * rows, PAD), rows)
        return mine_ref[at, :].astype(F32) + got_ref[at, :].astype(F32)

    send_ref[...] = part(1 - bit).astype(BF16)
    keep_ref[...] = part(bit)


def halve(mine, got, which):
    rows = mine.shape[0] // 2
    out = [jax.ShapeDtypeStruct((rows, TILE), BF16), jax.ShapeDtypeStruct((rows, TILE), F32)]
    return call(lambda *refs: halve_kernel(*refs, which=which), out, 2, mine, got)


def add_kernel(a_ref, b_ref, out_ref):
    out_ref[...] = (a_ref[...].astype(F32) + b_ref[...].astype(F32)).astype(BF16)


def add(a, b):
    return call(add_kernel, jax.ShapeDtypeStruct(a.shape, BF16), 2, a, b)


def join_kernel(mine_ref, got_ref, out_ref, *, which):
    rows = mine_ref.shape[0]
    bit = position()[which]
    out_ref[pl.ds(pl.multiple_of(bit * rows, PAD), rows), :] = mine_ref[...]
    out_ref[pl.ds(pl.multiple_of((1 - bit) * rows, PAD), rows), :] = got_ref[...]


def join(mine, got, which):
    out = jax.ShapeDtypeStruct((2 * mine.shape[0], TILE), BF16)
    return call(lambda *refs: join_kernel(*refs, which=which), out, 2, mine, got)


def share_kernel(a_ref, b_ref, out_ref, *, diagonal):
    rows = a_ref.shape[0]
    _, bit1, bit2 = position()
    offset = (2 * bit1 + bit2) * rows
    total = a_ref[...].astype(F32) + b_ref[...].astype(F32)
    out_ref[0:rows, :] = total.astype(BF16)
    square = total * total
    if diagonal:
        tile = (lax.broadcasted_iota(jnp.int32, (rows, TILE), 0) + offset) // TILE
        single = tile == diagonal[0]
        for at in diagonal[1:]:
            single |= tile == at
        square = jnp.where(single, square, 2.0 * square)
    else:
        square = 2.0 * square
    square = jnp.sum(jnp.sum(square, axis=0, keepdims=True), axis=1, keepdims=True)
    high = square.astype(BF16).astype(F32)
    rest = square - high
    middle = rest.astype(BF16).astype(F32)
    small = rest - middle
    line = lax.broadcasted_iota(jnp.int32, (PAD, TILE), 0)
    tail = jnp.where(line == 0, high, jnp.where(line == 1, middle, jnp.where(line == 2, small, 0.0)))
    out_ref[rows : rows + PAD, :] = tail.astype(BF16)


def make_share(a, b, diagonal):
    out = jax.ShapeDtypeStruct((a.shape[0] + PAD, TILE), BF16)
    return call(lambda *refs: share_kernel(*refs, diagonal=diagonal), out, 3, a, b)


def take_tile(ref, index):
    share_rows = ref.shape[0] // SHARES - PAD
    row, end = index * TILE, (index + 1) * TILE
    parts = []
    while row < end:
        share = row // share_rows
        stop = min(end, (share + 1) * share_rows)
        parts.append(ref[row + share * PAD : stop + share * PAD, :])
        row = stop
    return parts[0] if len(parts) == 1 else jnp.concatenate(parts, axis=0)


def put_block(ref, i, j, value):
    ref[i * TILE : (i + 1) * TILE, j * TILE : (j + 1) * TILE] = value


def near_kernel(orb_ref, vel_ref, own_ref, far_ref, out_ref, a_ref):
    side, _, near_at, _ = layout(orb_ref.shape[0])
    wide = side * TILE
    _, low, up = starts(0, side)
    for ref, at, n in ((own_ref, low, 0), (far_ref, up, 1)):
        for (i, j), index in near_at.items():
            value = take_tile(ref, index)
            put_block(a_ref, i + n * side, j, value)
            if i != j:
                put_block(a_ref, j + n * side, i, value.T)
        value = jnp.dot(
            a_ref[n * wide : (n + 1) * wide, :], orb_ref[pl.ds(at, wide), :], preferred_element_type=F32
        )
        out_ref[pl.ds(at, wide), :] = vel_ref[pl.ds(at, wide), :].astype(F32) - 0.5 * value


def apply_near(orb, vel, own, far):
    wide = orb.shape[0] // 2
    out = jax.ShapeDtypeStruct(orb.shape, F32)
    return call(near_kernel, out, 8, orb, vel, own, far, scratch=[pltpu.VMEM((2 * wide, wide), BF16)])


def tails(ref):
    share = ref.shape[0] // SHARES
    total = jnp.zeros((1, TILE), F32)
    for k in range(SHARES):
        lines = ref[(k + 1) * share - PAD : (k + 1) * share, :].astype(F32)
        total = total + jnp.sum(lines, axis=0, keepdims=True)
    return total


def far_kernel(orb_ref, base_ref, piece_ref, *refs, flip):
    total_rows = orb_ref.shape[0]
    side, extra, _, far_at = layout(total_rows)
    h, low, up = starts(flip, side)
    if len(refs) == 3:
        out_ref, b_ref, t_ref = refs
        copies = None
    else:
        near_own, near_far, own, hbm_ref, norm_ref, b_ref, t_ref, out_ref, sems = refs
        copies = []
        square = (tails(near_own) + tails(own)) + (tails(near_far) + tails(piece_ref))
        norm_ref[0] = (jnp.sqrt(square) / total_rows)[0, 0]
    zero = jnp.zeros((TILE, TILE), BF16)
    for i in range(side):
        for j in range(i, i - i % 2 + 2):
            if j < side:
                put_block(b_ref, i, j, zero)
                put_block(t_ref, j, i, zero)
    for (i, j), index in far_at.items():
        value = take_tile(piece_ref, index)
        put_block(b_ref, i, j, value)
        put_block(t_ref, j, i, value.T)
    for k in range(extra):
        value = take_tile(piece_ref, len(far_at) + k)
        at = pl.multiple_of((h * extra + k) * TILE, TILE)
        b_ref[pl.ds(at, TILE), pl.ds(at, TILE)] = value
        t_ref[pl.ds(at, TILE), pl.ds(at, TILE)] = value.T

    def put(at, value):
        out_ref[at, :] = base_ref[at, :] - 0.5 * value
        if copies is not None:
            copy = pltpu.make_async_copy(out_ref.at[at], hbm_ref.at[at], sems.at[len(copies)])
            copy.start()
            copies.append(copy)

    wide = side * TILE
    panel = 2 * TILE
    for p in range(0, wide, panel):
        end = min(p + panel, wide)
        value = jnp.dot(b_ref[p:end, :end], orb_ref[pl.ds(up, end), :], preferred_element_type=F32)
        put(pl.ds(pl.multiple_of(low + p, TILE), end - p), value)
        value = jnp.dot(t_ref[p:end, p:], orb_ref[pl.ds(low + p, wide - p), :], preferred_element_type=F32)
        put(pl.ds(pl.multiple_of(up + p, TILE), end - p), value)
    for copy in copies or ():
        copy.wait()


def apply_far(flip, orb, base, piece, others=()):
    wide = orb.shape[0] // 2
    out_shape = [jax.ShapeDtypeStruct(orb.shape, F32)]
    out_specs = [VMEM]
    scratch = [pltpu.VMEM((wide, wide), BF16)] * 2
    if others:
        out_shape.append(jax.ShapeDtypeStruct((1,), F32))
        out_specs = [pl.BlockSpec(memory_space=pltpu.HBM), SMEM]
        panels = -(-wide // (2 * TILE))
        scratch += [pltpu.VMEM(orb.shape, F32), pltpu.SemaphoreType.DMA((2 * panels,))]
    return pl.pallas_call(
        lambda *refs: far_kernel(*refs, flip=flip),
        out_shape=out_shape,
        in_specs=[VMEM] * (3 + len(others)),
        out_specs=out_specs,
        scratch_shapes=scratch,
        compiler_params=params(12 if others else 8),
    )(orb, base, piece, *others)


def pairs(nr, nc, even, odd):
    result = []
    for r in range(nr):
        for c in range(nc):
            on_r, on_c = odd if (c & 1) ^ parity(r, c) else even
            result.append((r * nc + c, (r ^ on_r) * nc + (c ^ on_c ^ parity(on_r, on_c))))
    return result


def local(orbitals, velocities):
    nr, nc = lax.axis_size("gr"), lax.axis_size("gc")
    side, _, near_at, _ = layout(orbitals.shape[0])
    swap = [(d, d ^ 1) for d in range(nr * nc)]
    first = pairs(nr, nc, (1, 0), (0, 2))
    second = pairs(nr, nc, (0, 2), (1, 0))
    rest = [(1 << b, 0) for b in range(1, nr.bit_length() - 1)]
    rest += [(0, 1 << b) for b in range(2, nc.bit_length() - 1)]
    doubling = [pairs(nr, nc, rest[k], rest[-1 - k]) for k in range(len(rest))]
    diagonals = [[near_at[(i, i)] for i in range(side)], []]

    def move(value, perm):
        return lax.ppermute(value, AXES, perm)

    joined = []
    for k in range(2):
        if k == 0:
            away, orbitals, velocities = load(orbitals, velocities)
        else:
            away = product(1, orbitals, velocities, k)
        got = move(away, swap)
        mine = product(0, orbitals, velocities, k)
        send, mine = halve(mine, got, 1)
        got = move(send, first)
        send, mine = halve(mine, got, 2)
        got = move(send, second)
        for perm in doubling:
            mine = add(mine, got)
            got = move(mine, perm)
        share = make_share(mine, got, diagonals[k])
        got = move(share, second)
        quarter = join(share, got, 2)
        got = move(quarter, first)
        joined.append(join(quarter, got, 1))
    far = [move(joined[k], swap) for k in range(2)]
    new = apply_near(orbitals, velocities, joined[0], far[0])
    (new,) = apply_far(0, orbitals, new, joined[1])
    new, measured = apply_far(1, orbitals, new, far[1], (joined[0], far[0], joined[1]))
    return new, measured


def solution(mesh):
    in_specs = (P(None, AXES), P(None, AXES))
    out_specs = (P(None, AXES), P())

    return jax.shard_map(local, mesh=mesh, in_specs=in_specs, out_specs=out_specs, check_vma=False)
```

```python
import jax
import jax.numpy as jnp
from jax import lax
from jax.experimental import pallas as pl
from jax.experimental.pallas import tpu as pltpu
from jax.sharding import PartitionSpec as P


TILE = 128
PAD = 16
SHARES = 4
CUTS = (16 / 39, 30 / 39)
TURNS = (0, 2, 1)
FAR_FIRST = 2
AXES = ("gr", "gc")
BF16 = jnp.bfloat16
F32 = jnp.float32
VMEM = pl.BlockSpec(memory_space=pltpu.VMEM)
SMEM = pl.BlockSpec(memory_space=pltpu.SMEM)
HBM = pl.BlockSpec(memory_space=pltpu.HBM)
DIMS = (((1,), (1,)), ((), ()))


def params(mib):
    return pltpu.CompilerParams(vmem_limit_bytes=mib * 2**20)


def call(kernel, out, mib, *operands, scratch=(), in_specs=None, out_specs=None):
    return pl.pallas_call(
        kernel,
        out_shape=out,
        in_specs=in_specs or [VMEM] * len(operands),
        out_specs=out_specs or jax.tree.map(lambda _: VMEM, out),
        scratch_shapes=scratch,
        compiler_params=params(mib),
    )(*operands)


def geometry(total_rows):
    side = total_rows // TILE // 2
    return side, side // 2


def chunk_tiles(total_rows):
    side, extra = geometry(total_rows)
    tiles = [("near", i, j) for j in range(side) for i in range(j + 1)]
    tiles += [("far", i, j) for j in range(side) for i in range(j + 1, side)]
    tiles += [("extra", k, k) for k in range(extra)]
    first, second = (round(cut * len(tiles)) for cut in CUTS)
    return [tiles[:first], tiles[first:second], tiles[second:]]


def parity(r, c):
    return (r ^ (r >> 1) ^ (c >> 1)) & 1


def pick(half, pair):
    return tuple(jnp.where(half == 0, a, b) for a, b in zip(*pair))


def position():
    r, c = lax.axis_index("gr"), lax.axis_index("gc")
    return r, c, (c & 1) ^ parity(r, c)


def side_bit(pair):
    r, c, half = position()
    on_r, on_c = pick(half, pair)
    return (((r & on_r) | (c & on_c)) != 0).astype(jnp.int32)


def starts(flip, side):
    _, _, half = position()
    h = half ^ flip
    low = pl.multiple_of(h * (side * TILE), TILE)
    up = pl.multiple_of((1 - h) * (side * TILE), TILE)
    return h, low, up


def symmetric(orb_ref, vel_ref, r0, rows, c0, cols):
    one = lax.dot_general(
        orb_ref[pl.ds(r0, rows), :], vel_ref[pl.ds(c0, cols), :], DIMS, preferred_element_type=F32
    )
    two = lax.dot_general(
        vel_ref[pl.ds(r0, rows), :], orb_ref[pl.ds(c0, cols), :], DIMS, preferred_element_type=F32
    )
    return one + two


def product_kernel(orb_ref, vel_ref, out_ref, *, flip, tiles, side, extra):
    h, low, up = starts(flip, side)
    for kind in ("near", "far"):
        table = {(i, j): n for n, (which, i, j) in enumerate(tiles) if which == kind}
        for c in range(0, side, 2):
            columns = [j for j in (c, c + 1) if any(at[1] == j for at in table)]
            if not columns:
                continue
            rows = [i for i in range(side) if any((i, j) in table for j in columns)]
            rows = list(range(rows[0], rows[-1] + 1))
            value = symmetric(
                orb_ref,
                vel_ref,
                low + rows[0] * TILE,
                len(rows) * TILE,
                (low if kind == "near" else up) + columns[0] * TILE,
                len(columns) * TILE,
            )
            for i in rows:
                for j in columns:
                    if (i, j) in table:
                        at = table[(i, j)] * TILE
                        row, col = (i - rows[0]) * TILE, (j - columns[0]) * TILE
                        out_ref[at : at + TILE, :] = value[row : row + TILE, col : col + TILE].astype(BF16)
    for n, (which, k, _) in enumerate(tiles):
        if which == "extra":
            shift = pl.multiple_of((h * extra + k) * TILE, TILE)
            value = symmetric(orb_ref, vel_ref, low + shift, TILE, up + shift, TILE)
            out_ref[n * TILE : (n + 1) * TILE, :] = value.astype(BF16)


def product(flip, orb, vel, tiles):
    side, extra = geometry(orb.shape[0])
    kernel = lambda *refs: product_kernel(*refs, flip=flip, tiles=tiles, side=side, extra=extra)
    return call(kernel, jax.ShapeDtypeStruct((len(tiles) * TILE, TILE), BF16), 6, orb, vel)


def load_kernel(orb_hbm, vel_hbm, away_ref, orb_ref, vel_ref, sems, *, tiles):
    total_rows = orb_hbm.shape[0]
    side, extra = geometry(total_rows)
    _, low, up = starts(1, side)
    rows = total_rows // 4
    copies = []
    for at in (low, low + rows, up, up + rows):
        for source, target in ((orb_hbm, orb_ref), (vel_hbm, vel_ref)):
            part = pl.ds(pl.multiple_of(at, TILE), rows)
            copies.append(pltpu.make_async_copy(source.at[part], target.at[part], sems.at[len(copies)]))
            copies[-1].start()
    for copy in copies[:4]:
        copy.wait()
    product_kernel(orb_ref, vel_ref, away_ref, flip=1, tiles=tiles, side=side, extra=extra)
    for copy in copies[4:]:
        copy.wait()


def load(orb, vel, tiles):
    whole = jax.ShapeDtypeStruct(orb.shape, orb.dtype)
    return call(
        lambda *refs: load_kernel(*refs, tiles=tiles),
        [jax.ShapeDtypeStruct((len(tiles) * TILE, TILE), BF16), whole, whole],
        12,
        pltpu.with_memory_space_constraint(orb, pltpu.HBM),
        pltpu.with_memory_space_constraint(vel, pltpu.HBM),
        scratch=[pltpu.SemaphoreType.DMA((8,))],
        in_specs=[HBM, HBM],
    )


def halve_kernel(mine_ref, got_ref, send_ref, keep_ref, *, pair):
    rows = send_ref.shape[0]
    bit = side_bit(pair)

    def part(index):
        at = pl.ds(pl.multiple_of(index * rows, PAD), rows)
        return mine_ref[at, :].astype(F32) + got_ref[at, :].astype(F32)

    send_ref[...] = part(1 - bit).astype(BF16)
    keep_ref[...] = part(bit)


def halve(mine, got, pair):
    rows = mine.shape[0] // 2
    out = [jax.ShapeDtypeStruct((rows, TILE), BF16), jax.ShapeDtypeStruct((rows, TILE), F32)]
    return call(lambda *refs: halve_kernel(*refs, pair=pair), out, 2, mine, got)


def add_kernel(a_ref, b_ref, out_ref):
    out_ref[...] = (a_ref[...].astype(F32) + b_ref[...].astype(F32)).astype(BF16)


def add(a, b):
    return call(add_kernel, jax.ShapeDtypeStruct(a.shape, BF16), 2, a, b)


def join_kernel(mine_ref, got_ref, out_ref, *, pair):
    rows = mine_ref.shape[0]
    bit = side_bit(pair)
    out_ref[pl.ds(pl.multiple_of(bit * rows, PAD), rows), :] = mine_ref[...]
    out_ref[pl.ds(pl.multiple_of((1 - bit) * rows, PAD), rows), :] = got_ref[...]


def join(mine, got, pair):
    out = jax.ShapeDtypeStruct((2 * mine.shape[0], TILE), BF16)
    return call(lambda *refs: join_kernel(*refs, pair=pair), out, 2, mine, got)


def share_kernel(a_ref, b_ref, out_ref, *, pairs, diagonal):
    rows = a_ref.shape[0]
    offset = (2 * side_bit(pairs[0]) + side_bit(pairs[1])) * rows
    total = a_ref[...].astype(F32) + b_ref[...].astype(F32)
    out_ref[0:rows, :] = total.astype(BF16)
    square = total * total
    if diagonal:
        tile = (lax.broadcasted_iota(jnp.int32, (rows, TILE), 0) + offset) // TILE
        single = tile == diagonal[0]
        for at in diagonal[1:]:
            single |= tile == at
        square = jnp.where(single, square, 2.0 * square)
    else:
        square = 2.0 * square
    square = jnp.sum(jnp.sum(square, axis=0, keepdims=True), axis=1, keepdims=True)
    high = square.astype(BF16).astype(F32)
    rest = square - high
    middle = rest.astype(BF16).astype(F32)
    small = rest - middle
    line = lax.broadcasted_iota(jnp.int32, (PAD, TILE), 0)
    tail = jnp.where(line == 0, high, jnp.where(line == 1, middle, jnp.where(line == 2, small, 0.0)))
    out_ref[rows : rows + PAD, :] = tail.astype(BF16)


def make_share(a, b, pairs, diagonal):
    out = jax.ShapeDtypeStruct((a.shape[0] + PAD, TILE), BF16)
    return call(lambda *refs: share_kernel(*refs, pairs=pairs, diagonal=diagonal), out, 3, a, b)


def take_tile(ref, index):
    share_rows = ref.shape[0] // SHARES - PAD
    row, end = index * TILE, (index + 1) * TILE
    parts = []
    while row < end:
        share = row // share_rows
        stop = min(end, (share + 1) * share_rows)
        parts.append(ref[row + share * PAD : stop + share * PAD, :])
        row = stop
    return parts[0] if len(parts) == 1 else jnp.concatenate(parts, axis=0)


def tails(refs):
    total = jnp.zeros((1, TILE), F32)
    for ref in refs:
        share = ref.shape[0] // SHARES
        for k in range(SHARES):
            lines = ref[(k + 1) * share - PAD : (k + 1) * share, :].astype(F32)
            total = total + jnp.sum(lines, axis=0, keepdims=True)
    return total


def put_block(ref, i, j, value):
    ref[i * TILE : (i + 1) * TILE, j * TILE : (j + 1) * TILE] = value


def piece_values(piece_ref, tiles, flip, orb_ref, mats, side, extra):
    h, low, up = starts(flip, side)
    near_ref, far_ref, flip_ref = mats
    near, far, back = {}, {}, {}
    extras = []
    for n, (which, i, j) in enumerate(tiles):
        if which == "near":
            near[(i, j)] = (n, False)
            if i != j:
                near[(j, i)] = (n, True)
        elif which == "far":
            far[(i, j)] = (n, False)
            back[(j, i)] = (n, True)
        else:
            extras.append((n, i))
    for table in (far, back):
        if extras:
            for i in range(side):
                table[(i, i)] = None
    spans = {}
    zero = jnp.zeros((TILE, TILE), BF16)
    for name, ref, table in (("near", near_ref, near), ("far", far_ref, far), ("back", flip_ref, back)):
        for p in range(0, side, 2):
            rows = range(p, min(p + 2, side))
            columns = [j for (i, j) in table if i in rows]
            if not columns:
                continue
            span = (min(columns), max(columns) + 1)
            spans[(name, p)] = span
            for i in rows:
                for j in range(*span):
                    if table.get((i, j)) is None:
                        put_block(ref, i, j, zero)
    for (i, j), (n, turned) in near.items():
        if not turned:
            value = take_tile(piece_ref, n)
            put_block(near_ref, i, j, value)
            if i != j:
                put_block(near_ref, j, i, value.T)
    for (i, j), entry in far.items():
        if entry is not None:
            value = take_tile(piece_ref, entry[0])
            put_block(far_ref, i, j, value)
            put_block(flip_ref, j, i, value.T)
    for n, k in extras:
        value = take_tile(piece_ref, n)
        at = pl.ds(pl.multiple_of((h * extra + k) * TILE, TILE), TILE)
        far_ref[at, at] = value
        flip_ref[at, at] = value.T

    def part(name, ref, p, base):
        if (name, p) not in spans:
            return None
        begin, end = spans[(name, p)]
        left = ref[p * TILE : min(p + 2, side) * TILE, begin * TILE : end * TILE]
        right = orb_ref[pl.ds(pl.multiple_of(base + begin * TILE, TILE), (end - begin) * TILE), :]
        return jnp.dot(left, right, preferred_element_type=F32)

    for p in range(0, side, 2):
        one, two = part("near", near_ref, p, low), part("far", far_ref, p, up)
        if one is not None or two is not None:
            yield flip, p, one if two is None else two if one is None else one + two
    for p in range(0, side, 2):
        value = part("back", flip_ref, p, low)
        if value is not None:
            yield 1 - flip, p, value


def apply_kernel(*refs, plan, blocks, side, extra, last):
    refs = list(refs)
    orb_ref = refs.pop(0)
    vel_ref = refs.pop(0) if blocks["vel"] else None
    bases = {b: refs.pop(0) for b in blocks["in"]}
    pieces = [refs.pop(0) for _ in plan]
    if last:
        squares = [refs.pop(0) for _ in range(blocks["squares"])]
        out_hbm, norm_ref = refs.pop(0), refs.pop(0)
        scratch = refs.pop(0)
        outs = {b: scratch.at[b] for b in (0, 1)}
    else:
        outs = {b: refs.pop(0) for b in blocks["out"]}
    mats = refs[:3]
    _, low, up = starts(0, side)
    base_row = (low, up)
    written = set()
    copies = []

    def rows_of(p):
        return slice(p * TILE, min(p + 2, side) * TILE)

    def before(b, p):
        if (b, p) in written:
            return outs[b][rows_of(p), :]
        if b in bases:
            return bases[b][rows_of(p), :]
        rows = rows_of(p)
        at = pl.ds(pl.multiple_of(base_row[b] + rows.start, TILE), rows.stop - rows.start)
        return vel_ref[at, :].astype(F32)

    def send(source, b, p):
        rows = rows_of(p)
        at = pl.ds(pl.multiple_of(base_row[b] + rows.start, TILE), rows.stop - rows.start)
        copy = pltpu.make_async_copy(source.at[rows], out_hbm.at[at], refs[3].at[len(copies)])
        copy.start()
        copies.append(copy)

    if last:
        (tiles, flip), piece = plan[0], pieces[0]
        touched = {("near", i // 2 * 2) for which, i, j in tiles if which == "near"}
        touched |= {("near", j // 2 * 2) for which, i, j in tiles if which == "near"}
        touched |= {("near", i // 2 * 2) for which, i, j in tiles if which == "far"}
        touched |= {("back", j // 2 * 2) for which, i, j in tiles if which == "far"}
        if any(which == "extra" for which, _, _ in tiles):
            touched |= {(name, p) for name in ("near", "back") for p in range(0, side, 2)}
        for b, name in ((flip, "near"), (1 - flip, "back")):
            for p in range(0, side, 2):
                if (name, p) not in touched:
                    send(bases[b], b, p)
    for (tiles, flip), piece in zip(plan, pieces):
        for b, p, value in piece_values(piece, tiles, flip, orb_ref, mats, side, extra):
            outs[b][rows_of(p), :] = before(b, p) - 0.5 * value
            written.add((b, p))
            if last:
                send(outs[b], b, p)
    if last:
        count = len(squares) // 2
        square = tails(squares[:count]) + tails(squares[count:])
        norm_ref[0] = (jnp.sqrt(square) / (2 * side * TILE))[0, 0]
        for copy in copies:
            copy.wait()
    else:
        for b in outs:
            for p in range(0, side, 2):
                if (b, p) not in written:
                    outs[b][rows_of(p), :] = before(b, p)


def apply(orb, vel, bases, plan, pieces, squares=None):
    side, extra = geometry(orb.shape[0])
    wide, columns = side * TILE, orb.shape[1]
    last = squares is not None
    touched = set()
    for tiles, flip in plan:
        touched.add(flip)
        if any(which != "near" for which, _, _ in tiles):
            touched.add(1 - flip)
    given = [b for b in (0, 1) if bases[b] is not None and (b in touched or last)]
    blocks = {"in": given, "out": sorted(touched), "vel": any(bases[b] is None for b in touched)}
    operands = [orb] + ([vel] if blocks["vel"] else []) + [bases[b] for b in given] + list(pieces)
    mats = [pltpu.VMEM((wide, wide), BF16)] * 3
    if last:
        blocks["squares"] = len(squares)
        operands += squares
        panels = 2 * -(-side // 2)
        return call(
            lambda *refs: apply_kernel(*refs, plan=plan, blocks=blocks, side=side, extra=extra, last=True),
            [jax.ShapeDtypeStruct(orb.shape, F32), jax.ShapeDtypeStruct((1,), F32)],
            14,
            *operands,
            scratch=[pltpu.VMEM((2, wide, columns), F32)] + mats + [pltpu.SemaphoreType.DMA((panels,))],
            out_specs=[HBM, SMEM],
        )
    outs = call(
        lambda *refs: apply_kernel(*refs, plan=plan, blocks=blocks, side=side, extra=extra, last=False),
        [jax.ShapeDtypeStruct((wide, columns), F32)] * len(touched),
        10,
        *operands,
        scratch=mats,
    )
    result = list(bases)
    for b, value in zip(sorted(touched), outs):
        result[b] = value
    return result


def permutation(nr, nc, pair):
    result = []
    for r in range(nr):
        for c in range(nc):
            on_r, on_c = pair[(c & 1) ^ parity(r, c)]
            result.append((r * nc + c, (r ^ on_r) * nc + (c ^ on_c ^ parity(on_r, on_c))))
    return result


def routes(nr, nc):
    low = [(1, 0), (0, 2)]
    rest = [(1 << b, 0) for b in range(1, nr.bit_length() - 1)]
    rest += [(0, 1 << b) for b in range(2, nc.bit_length() - 1)]

    def both_ways(bits):
        return list(zip(bits, bits[::-1]))

    usual = (both_ways(low), both_ways(rest))
    result = [usual] * 3
    if len(rest) > 1:
        result[FAR_FIRST] = (both_ways([rest[0], rest[-1]]), both_ways(low + rest[1:-1]))
    return result


def local(orbitals, velocities):
    nr, nc = lax.axis_size("gr"), lax.axis_size("gc")
    _, _ = geometry(orbitals.shape[0])
    chunks = chunk_tiles(orbitals.shape[0])
    plans = routes(nr, nc)
    swap = [(d, d ^ 1) for d in range(nr * nc)]
    joined, far = {}, {}
    for k in TURNS:
        tiles = chunks[k]
        halvings, doublings = plans[k]
        diagonal = [n for n, (which, i, j) in enumerate(tiles) if which == "near" and i == j]

        def move(value, pair):
            return lax.ppermute(value, AXES, swap if pair is None else permutation(nr, nc, pair))

        if k == TURNS[0]:
            send, orbitals, velocities = load(orbitals, velocities, tiles)
        else:
            send = product(1, orbitals, velocities, tiles)
        got = move(send, None)
        mine = product(0, orbitals, velocities, tiles)
        for pair in halvings:
            send, mine = halve(mine, got, pair)
            got = move(send, pair)
        for pair in doublings:
            mine = add(mine, got)
            got = move(mine, pair)
        mine = make_share(mine, got, halvings, diagonal)
        for pair in halvings[::-1]:
            got = move(mine, pair)
            mine = join(mine, got, pair)
        joined[k] = mine
        far[k] = move(mine, None)
    first, second, third = TURNS
    blocks = [None, None]
    blocks = apply(orbitals, velocities, blocks, [(chunks[first], 0)], [joined[first]])
    plan = [(chunks[first], 1), (chunks[second], 0)]
    blocks = apply(orbitals, velocities, blocks, plan, [far[first], joined[second]])
    plan = [(chunks[second], 1), (chunks[third], 0)]
    blocks = apply(orbitals, velocities, blocks, plan, [far[second], joined[third]])
    squares = [joined[k] for k in TURNS] + [far[k] for k in TURNS]
    return tuple(apply(orbitals, velocities, blocks, [(chunks[third], 1)], [far[third]], squares))


def solution(mesh):
    in_specs = (P(None, AXES), P(None, AXES))
    out_specs = (P(None, AXES), P())

    return jax.shard_map(local, mesh=mesh, in_specs=in_specs, out_specs=out_specs, check_vma=False)
```

```python
import jax
import jax.numpy as jnp
from jax import lax
from jax.experimental import pallas as pl
from jax.experimental.pallas import tpu as pltpu
from jax.sharding import PartitionSpec as P


TILE = 128
PAD = 16
SHARES = 4
CUTS = (17 / 39, 31 / 39)
TURNS = (0, 1, 2)
FAR_FIRST = 2
AXES = ("gr", "gc")
BF16 = jnp.bfloat16
F32 = jnp.float32
VMEM = pl.BlockSpec(memory_space=pltpu.VMEM)
SMEM = pl.BlockSpec(memory_space=pltpu.SMEM)
HBM = pl.BlockSpec(memory_space=pltpu.HBM)
DIMS = (((1,), (1,)), ((), ()))


def params(mib):
    return pltpu.CompilerParams(vmem_limit_bytes=mib * 2**20)


def call(kernel, out, mib, *operands, scratch=(), in_specs=None, out_specs=None):
    return pl.pallas_call(
        kernel,
        out_shape=out,
        in_specs=in_specs or [VMEM] * len(operands),
        out_specs=out_specs or jax.tree.map(lambda _: VMEM, out),
        scratch_shapes=scratch,
        compiler_params=params(mib),
    )(*operands)


def geometry(total_rows):
    side = total_rows // TILE // 2
    return side, side // 2


def chunk_tiles(total_rows):
    side, extra = geometry(total_rows)
    tiles = [("near", i, j) for j in range(side) for i in range(j + 1)]
    tiles += [("far", i, j) for j in range(side) for i in range(j + 1, side)]
    tiles += [("extra", k, k) for k in range(extra)]
    first, second = (round(cut * len(tiles)) for cut in CUTS)
    return [tiles[:first], tiles[first:second], tiles[second:]]


def parity(r, c):
    return (r ^ (r >> 1) ^ (c >> 1)) & 1


def pick(half, pair):
    return tuple(jnp.where(half == 0, a, b) for a, b in zip(*pair))


def position():
    r, c = lax.axis_index("gr"), lax.axis_index("gc")
    return r, c, (c & 1) ^ parity(r, c)


def side_bit(pair):
    r, c, half = position()
    on_r, on_c = pick(half, pair)
    return (((r & on_r) | (c & on_c)) != 0).astype(jnp.int32)


def starts(flip, side):
    _, _, half = position()
    h = half ^ flip
    low = pl.multiple_of(h * (side * TILE), TILE)
    up = pl.multiple_of((1 - h) * (side * TILE), TILE)
    return h, low, up


def symmetric(orb_ref, vel_ref, r0, rows, c0, cols):
    one = lax.dot_general(
        orb_ref[pl.ds(r0, rows), :], vel_ref[pl.ds(c0, cols), :], DIMS, preferred_element_type=F32
    )
    two = lax.dot_general(
        vel_ref[pl.ds(r0, rows), :], orb_ref[pl.ds(c0, cols), :], DIMS, preferred_element_type=F32
    )
    return one + two


def product_kernel(orb_ref, vel_ref, out_ref, *, flip, tiles, side, extra):
    h, low, up = starts(flip, side)
    for kind in ("near", "far"):
        table = {(i, j): n for n, (which, i, j) in enumerate(tiles) if which == kind}
        for c in range(0, side, 2):
            columns = [j for j in (c, c + 1) if any(at[1] == j for at in table)]
            if not columns:
                continue
            rows = [i for i in range(side) if any((i, j) in table for j in columns)]
            rows = list(range(rows[0], rows[-1] + 1))
            value = symmetric(
                orb_ref,
                vel_ref,
                low + rows[0] * TILE,
                len(rows) * TILE,
                (low if kind == "near" else up) + columns[0] * TILE,
                len(columns) * TILE,
            )
            for i in rows:
                for j in columns:
                    if (i, j) in table:
                        at = table[(i, j)] * TILE
                        row, col = (i - rows[0]) * TILE, (j - columns[0]) * TILE
                        out_ref[at : at + TILE, :] = value[row : row + TILE, col : col + TILE].astype(BF16)
    for n, (which, k, _) in enumerate(tiles):
        if which == "extra":
            shift = pl.multiple_of((h * extra + k) * TILE, TILE)
            value = symmetric(orb_ref, vel_ref, low + shift, TILE, up + shift, TILE)
            out_ref[n * TILE : (n + 1) * TILE, :] = value.astype(BF16)


def product(flip, orb, vel, tiles):
    side, extra = geometry(orb.shape[0])
    kernel = lambda *refs: product_kernel(*refs, flip=flip, tiles=tiles, side=side, extra=extra)
    return call(kernel, jax.ShapeDtypeStruct((len(tiles) * TILE, TILE), BF16), 6, orb, vel)


def load_kernel(orb_hbm, vel_hbm, away_ref, orb_ref, vel_ref, sems, *, tiles):
    total_rows = orb_hbm.shape[0]
    side, extra = geometry(total_rows)
    _, low, up = starts(1, side)
    rows = total_rows // 4
    copies = []
    for at in (low, low + rows, up, up + rows):
        for source, target in ((orb_hbm, orb_ref), (vel_hbm, vel_ref)):
            part = pl.ds(pl.multiple_of(at, TILE), rows)
            copies.append(pltpu.make_async_copy(source.at[part], target.at[part], sems.at[len(copies)]))
            copies[-1].start()
    for copy in copies[:4]:
        copy.wait()
    product_kernel(orb_ref, vel_ref, away_ref, flip=1, tiles=tiles, side=side, extra=extra)
    for copy in copies[4:]:
        copy.wait()


def load(orb, vel, tiles):
    whole = jax.ShapeDtypeStruct(orb.shape, orb.dtype)
    return call(
        lambda *refs: load_kernel(*refs, tiles=tiles),
        [jax.ShapeDtypeStruct((len(tiles) * TILE, TILE), BF16), whole, whole],
        12,
        pltpu.with_memory_space_constraint(orb, pltpu.HBM),
        pltpu.with_memory_space_constraint(vel, pltpu.HBM),
        scratch=[pltpu.SemaphoreType.DMA((8,))],
        in_specs=[HBM, HBM],
    )


def halve_kernel(mine_ref, got_ref, send_ref, keep_ref, *, pair):
    rows = send_ref.shape[0]
    bit = side_bit(pair)

    def part(index):
        at = pl.ds(pl.multiple_of(index * rows, PAD), rows)
        return mine_ref[at, :].astype(F32) + got_ref[at, :].astype(F32)

    send_ref[...] = part(1 - bit).astype(BF16)
    keep_ref[...] = part(bit)


def halve(mine, got, pair):
    rows = mine.shape[0] // 2
    out = [jax.ShapeDtypeStruct((rows, TILE), BF16), jax.ShapeDtypeStruct((rows, TILE), F32)]
    return call(lambda *refs: halve_kernel(*refs, pair=pair), out, 2, mine, got)


def add_kernel(a_ref, b_ref, out_ref):
    out_ref[...] = (a_ref[...].astype(F32) + b_ref[...].astype(F32)).astype(BF16)


def add(a, b):
    return call(add_kernel, jax.ShapeDtypeStruct(a.shape, BF16), 2, a, b)


def join_kernel(mine_ref, got_ref, out_ref, *, pair):
    rows = mine_ref.shape[0]
    bit = side_bit(pair)
    out_ref[pl.ds(pl.multiple_of(bit * rows, PAD), rows), :] = mine_ref[...]
    out_ref[pl.ds(pl.multiple_of((1 - bit) * rows, PAD), rows), :] = got_ref[...]


def join(mine, got, pair):
    out = jax.ShapeDtypeStruct((2 * mine.shape[0], TILE), BF16)
    return call(lambda *refs: join_kernel(*refs, pair=pair), out, 2, mine, got)


def share_kernel(a_ref, b_ref, out_ref, *, pairs, diagonal):
    rows = a_ref.shape[0]
    offset = (2 * side_bit(pairs[0]) + side_bit(pairs[1])) * rows
    total = a_ref[...].astype(F32) + b_ref[...].astype(F32)
    out_ref[0:rows, :] = total.astype(BF16)
    square = total * total
    if diagonal:
        tile = (lax.broadcasted_iota(jnp.int32, (rows, TILE), 0) + offset) >> (TILE.bit_length() - 1)
        single = tile == diagonal[0]
        for at in diagonal[1:]:
            single |= tile == at
        square = jnp.where(single, square, 2.0 * square)
    else:
        square = 2.0 * square
    square = jnp.sum(jnp.sum(square, axis=0, keepdims=True), axis=1, keepdims=True)
    high = square.astype(BF16).astype(F32)
    rest = square - high
    middle = rest.astype(BF16).astype(F32)
    small = rest - middle
    line = lax.broadcasted_iota(jnp.int32, (PAD, TILE), 0)
    tail = jnp.where(line == 0, high, jnp.where(line == 1, middle, jnp.where(line == 2, small, 0.0)))
    out_ref[rows : rows + PAD, :] = tail.astype(BF16)


def make_share(a, b, pairs, diagonal):
    out = jax.ShapeDtypeStruct((a.shape[0] + PAD, TILE), BF16)
    return call(lambda *refs: share_kernel(*refs, pairs=pairs, diagonal=diagonal), out, 3, a, b)


def take_tile(ref, index):
    share_rows = ref.shape[0] // SHARES - PAD
    row, end = index * TILE, (index + 1) * TILE
    parts = []
    while row < end:
        share = row // share_rows
        stop = min(end, (share + 1) * share_rows)
        parts.append(ref[row + share * PAD : stop + share * PAD, :])
        row = stop
    return parts[0] if len(parts) == 1 else jnp.concatenate(parts, axis=0)


def tails(refs):
    total = jnp.zeros((1, TILE), F32)
    for ref in refs:
        share = ref.shape[0] // SHARES
        for k in range(SHARES):
            lines = ref[(k + 1) * share - PAD : (k + 1) * share, :].astype(F32)
            total = total + jnp.sum(lines, axis=0, keepdims=True)
    return total


def put_block(ref, i, j, value):
    ref[i * TILE : (i + 1) * TILE, j * TILE : (j + 1) * TILE] = value


def tables(tiles, side):
    result = {"near": {}, "far": {}, "back": {}}
    for n, (which, i, j) in enumerate(tiles):
        if which == "near":
            result["near"][(i, j)] = n
            result["near"][(j, i)] = n
        elif which == "far":
            result["far"][(i, j)] = n
            result["back"][(j, i)] = n
    if any(which == "extra" for which, _, _ in tiles):
        for name in ("far", "back"):
            for i in range(side):
                result[name][(i, i)] = None
    return {name: table for name, table in result.items() if table}


def spans_of(table, side):
    spans = {}
    for p in range(0, side, 2):
        columns = [j for (i, j) in table if i in (p, p + 1)]
        if columns:
            spans[p] = (min(columns), max(columns) + 1)
    return spans


def reach(tiles, flip, side):
    result = set()
    for name, table in tables(tiles, side).items():
        result |= {(1 - flip if name == "back" else flip, p) for p in spans_of(table, side)}
    return result


def fill(piece_ref, tiles, flip, mats, side, extra):
    h, low, up = starts(flip, side)
    found = tables(tiles, side)
    zero = jnp.zeros((TILE, TILE), BF16)
    terms = {}
    for name, table in found.items():
        ref = mats[name]
        for p, (begin, end) in spans_of(table, side).items():
            last = min(p + 2, side)
            for i in range(p, last):
                for j in range(begin, end):
                    if table.get((i, j)) is None:
                        put_block(ref, i, j, zero)
            key = (1 - flip if name == "back" else flip, p)
            left = (slice(p * TILE, last * TILE), slice(begin * TILE, end * TILE))
            base = up if name == "far" else low
            terms.setdefault(key, []).append((ref, left, base + begin * TILE, (end - begin) * TILE))
    for n, (which, i, j) in enumerate(tiles):
        value = take_tile(piece_ref, n)
        if which == "near":
            put_block(mats["near"], i, j, value)
            if i != j:
                put_block(mats["near"], j, i, value.T)
        elif which == "far":
            put_block(mats["far"], i, j, value)
            put_block(mats["back"], j, i, value.T)
        else:
            at = pl.ds(pl.multiple_of((h * extra + i) * TILE, TILE), TILE)
            mats["far"][at, at] = value
            mats["back"][at, at] = value.T
    return terms


def apply_kernel(*refs, plan, given, velocities, count, side, extra, names):
    refs = list(refs)
    orb_ref = refs.pop(0)
    vel_ref = refs.pop(0) if velocities else None
    bases = {b: refs.pop(0) for b in given}
    pieces = [refs.pop(0) for _ in plan]
    touched = set().union(*(reach(tiles, flip, side) for tiles, flip in plan))
    last = count > 0
    copies = []
    if last:
        squares = [refs.pop(0) for _ in range(count)]
        out_hbm, norm_ref, scratch, sems = refs.pop(0), refs.pop(0), refs.pop(0), refs.pop()
        outs = {b: scratch.at[b] for b in (0, 1)}
    else:
        outs = {b: refs.pop(0) for b in sorted({b for b, _ in touched})}
    _, low, up = starts(0, side)
    base_row = (low, up)

    def rows_of(p):
        return slice(p * TILE, min(p + 2, side) * TILE)

    def place(b, p):
        rows = rows_of(p)
        return pl.ds(pl.multiple_of(base_row[b] + rows.start, TILE), rows.stop - rows.start)

    def before(b, p):
        return bases[b][rows_of(p), :] if b in bases else vel_ref[place(b, p), :].astype(F32)

    def send(source, b, p):
        copy = pltpu.make_async_copy(source.at[rows_of(p)], out_hbm.at[place(b, p)], sems.at[len(copies)])
        copy.start()
        copies.append(copy)

    for b in outs:
        for p in range(0, side, 2):
            if (b, p) not in touched:
                if last:
                    send(bases[b], b, p)
                else:
                    outs[b][rows_of(p), :] = before(b, p)
    terms = {}
    for (tiles, flip), piece, own in zip(plan, pieces, names):
        mats = {name: refs.pop(0) for name in own}
        for key, value in fill(piece, tiles, flip, mats, side, extra).items():
            terms.setdefault(key, []).extend(value)
    for b, p in sorted(touched):
        total = None
        for ref, left, at, rows in terms[(b, p)]:
            right = orb_ref[pl.ds(pl.multiple_of(at, TILE), rows), :]
            value = jnp.dot(ref[left], right, preferred_element_type=F32)
            total = value if total is None else total + value
        outs[b][rows_of(p), :] = before(b, p) - 0.5 * total
        if last:
            send(outs[b], b, p)
    if last:
        square = tails(squares[: count // 2]) + tails(squares[count // 2 :])
        norm_ref[0] = (jnp.sqrt(square) / (2 * side * TILE))[0, 0]
        for copy in copies:
            copy.wait()


def apply(orb, vel, bases, plan, pieces, squares=()):
    side, extra = geometry(orb.shape[0])
    wide, columns = side * TILE, orb.shape[1]
    blocks = [0, 1] if squares else sorted({b for tiles, flip in plan for b, _ in reach(tiles, flip, side)})
    given = [b for b in blocks if bases[b] is not None]
    velocities = len(given) < len(blocks)
    names = [list(tables(tiles, side)) for tiles, _ in plan]
    mats = [pltpu.VMEM((wide, wide), BF16) for own in names for _ in own]
    kernel = lambda *refs: apply_kernel(
        *refs,
        plan=plan,
        given=given,
        velocities=velocities,
        count=len(squares),
        side=side,
        extra=extra,
        names=names,
    )
    operands = [orb] + ([vel] if velocities else []) + [bases[b] for b in given] + list(pieces) + list(squares)
    if squares:
        return call(
            kernel,
            [jax.ShapeDtypeStruct(orb.shape, F32), jax.ShapeDtypeStruct((1,), F32)],
            14,
            *operands,
            scratch=[pltpu.VMEM((2, wide, columns), F32)] + mats + [pltpu.SemaphoreType.DMA((2 * -(-side // 2),))],
            out_specs=[HBM, SMEM],
        )
    out = [jax.ShapeDtypeStruct((wide, columns), F32)] * len(blocks)
    values = call(kernel, out, 8 + 2 * len(mats), *operands, scratch=mats)
    result = list(bases)
    for b, value in zip(blocks, values):
        result[b] = value
    return result


def permutation(nr, nc, pair):
    result = []
    for r in range(nr):
        for c in range(nc):
            on_r, on_c = pair[(c & 1) ^ parity(r, c)]
            result.append((r * nc + c, (r ^ on_r) * nc + (c ^ on_c ^ parity(on_r, on_c))))
    return result


def routes(nr, nc):
    low = [(1, 0), (0, 2)]
    rest = [(1 << b, 0) for b in range(1, nr.bit_length() - 1)]
    rest += [(0, 1 << b) for b in range(2, nc.bit_length() - 1)]

    def both_ways(bits):
        return list(zip(bits, bits[::-1]))

    usual = (both_ways(low), both_ways(rest))
    result = [usual] * 3
    if len(rest) > 1:
        result[FAR_FIRST] = (both_ways([rest[0], rest[-1]]), both_ways(low + rest[1:-1]))
    return result


def local(orbitals, velocities):
    nr, nc = lax.axis_size("gr"), lax.axis_size("gc")
    _, _ = geometry(orbitals.shape[0])
    chunks = chunk_tiles(orbitals.shape[0])
    plans = routes(nr, nc)
    swap = [(d, d ^ 1) for d in range(nr * nc)]
    joined, far = {}, {}
    for k in TURNS:
        tiles = chunks[k]
        halvings, doublings = plans[k]
        diagonal = [n for n, (which, i, j) in enumerate(tiles) if which == "near" and i == j]

        def move(value, pair):
            return lax.ppermute(value, AXES, swap if pair is None else permutation(nr, nc, pair))

        if k == TURNS[0]:
            send, orbitals, velocities = load(orbitals, velocities, tiles)
        else:
            send = product(1, orbitals, velocities, tiles)
        got = move(send, None)
        mine = product(0, orbitals, velocities, tiles)
        for pair in halvings:
            send, mine = halve(mine, got, pair)
            got = move(send, pair)
        for pair in doublings:
            mine = add(mine, got)
            got = move(mine, pair)
        mine = make_share(mine, got, halvings, diagonal)
        for pair in halvings[::-1]:
            got = move(mine, pair)
            mine = join(mine, got, pair)
        joined[k] = mine
        far[k] = move(mine, None)
    first, second, third = TURNS
    blocks = [None, None]
    blocks = apply(orbitals, velocities, blocks, [(chunks[first], 0)], [joined[first]])
    blocks = apply(orbitals, velocities, blocks, [(chunks[first], 1)], [far[first]])
    plan = [(chunks[second], 0), (chunks[second], 1), (chunks[third], 0)]
    blocks = apply(orbitals, velocities, blocks, plan, [joined[second], far[second], joined[third]])
    squares = [joined[k] for k in TURNS] + [far[k] for k in TURNS]
    return tuple(apply(orbitals, velocities, blocks, [(chunks[third], 1)], [far[third]], squares))


def solution(mesh):
    in_specs = (P(None, AXES), P(None, AXES))
    out_specs = (P(None, AXES), P())

    return jax.shard_map(local, mesh=mesh, in_specs=in_specs, out_specs=out_specs, check_vma=False)
```

```python
import jax
import jax.numpy as jnp
from jax import lax
from jax.experimental import pallas as pl
from jax.experimental.pallas import tpu as pltpu
from jax.sharding import PartitionSpec as P


TILE = 128
PAD = 16
SHARES = 4
CUT = 17 / 39
LATE = (2, 2)
TURNS = (0, 1, 2)
FAR_FIRST = 2
TWO = 1
PIECE = 128
PANEL = 2
AXES = ("gr", "gc")
BF16 = jnp.bfloat16
F32 = jnp.float32
VMEM = pl.BlockSpec(memory_space=pltpu.VMEM)
SMEM = pl.BlockSpec(memory_space=pltpu.SMEM)
HBM = pl.BlockSpec(memory_space=pltpu.HBM)
DIMS = (((1,), (1,)), ((), ()))


def params(mib):
    return pltpu.CompilerParams(vmem_limit_bytes=mib * 2**20)


def call(kernel, out, mib, *operands, scratch=(), in_specs=None, out_specs=None, aliases={}):
    return pl.pallas_call(
        kernel,
        out_shape=out,
        in_specs=in_specs or [VMEM] * len(operands),
        out_specs=out_specs or jax.tree.map(lambda _: VMEM, out),
        scratch_shapes=scratch,
        input_output_aliases=aliases,
        compiler_params=params(mib),
    )(*operands)


def geometry(total_rows):
    side = total_rows // TILE // 2
    return side, side // 2


def chunk_tiles(total_rows):
    side, extra = geometry(total_rows)
    near = [("near", i, j) for j in range(side) for i in range(j + 1)]
    far = [("far", i, j) for j in range(side) for i in range(j + 1, side)]
    late = [at for at in near if at[1] >= side - LATE[0] and at[2] == side - 1] + [at for at in far if at[2] >= LATE[1]]
    tiles = [at for at in near if at not in late]
    tiles += [("extra", k, k) for k in range(extra)]
    tiles += [at for at in far if at not in late]
    cut = round(CUT * (len(tiles) + len(late)))
    return [tiles[:cut], tiles[cut:], late]


def parity(r, c):
    return (r ^ (r >> 1) ^ (c >> 1)) & 1


def pick(half, pair):
    return tuple(jnp.where(half == 0, a, b) for a, b in zip(*pair))


def position():
    r, c = lax.axis_index("gr"), lax.axis_index("gc")
    return r, c, (c & 1) ^ parity(r, c)


def side_bit(pair):
    r, c, half = position()
    on_r, on_c = pick(half, pair)
    return (((r & on_r) | (c & on_c)) != 0).astype(jnp.int32)


def starts(flip, side):
    _, _, half = position()
    h = half ^ flip
    low = pl.multiple_of(h * (side * TILE), TILE)
    up = pl.multiple_of((1 - h) * (side * TILE), TILE)
    return h, low, up


def symmetric(orb_ref, vel_ref, r0, rows, c0, cols):
    one = lax.dot_general(
        orb_ref[pl.ds(r0, rows), :], vel_ref[pl.ds(c0, cols), :], DIMS, preferred_element_type=F32
    )
    two = lax.dot_general(
        vel_ref[pl.ds(r0, rows), :], orb_ref[pl.ds(c0, cols), :], DIMS, preferred_element_type=F32
    )
    return one + two


def product_kernel(orb_ref, vel_ref, out_ref, *, flip, tiles, side, extra):
    h, low, up = starts(flip, side)
    for kind in ("near", "far"):
        table = {(i, j): n for n, (which, i, j) in enumerate(tiles) if which == kind}
        for c in range(0, side, 2):
            columns = [j for j in (c, c + 1) if any(at[1] == j for at in table)]
            if not columns:
                continue
            rows = [i for i in range(side) if any((i, j) in table for j in columns)]
            rows = list(range(rows[0], rows[-1] + 1))
            value = symmetric(
                orb_ref,
                vel_ref,
                low + rows[0] * TILE,
                len(rows) * TILE,
                (low if kind == "near" else up) + columns[0] * TILE,
                len(columns) * TILE,
            )
            for i in rows:
                for j in columns:
                    if (i, j) in table:
                        at = table[(i, j)] * TILE
                        row, col = (i - rows[0]) * TILE, (j - columns[0]) * TILE
                        out_ref[at : at + TILE, :] = value[row : row + TILE, col : col + TILE].astype(BF16)
    for n, (which, k, _) in enumerate(tiles):
        if which == "extra":
            shift = pl.multiple_of((h * extra + k) * TILE, TILE)
            value = symmetric(orb_ref, vel_ref, low + shift, TILE, up + shift, TILE)
            out_ref[n * TILE : (n + 1) * TILE, :] = value.astype(BF16)


def product(flip, orb, vel, tiles):
    side, extra = geometry(orb.shape[0])
    kernel = lambda *refs: product_kernel(*refs, flip=flip, tiles=tiles, side=side, extra=extra)
    return call(kernel, jax.ShapeDtypeStruct((len(tiles) * TILE, TILE), BF16), 6, orb, vel)


def load_kernel(orb_hbm, vel_hbm, away_ref, orb_ref, vel_ref, sems, *, tiles):
    total_rows = orb_hbm.shape[0]
    side, extra = geometry(total_rows)
    _, low, up = starts(1, side)
    rows = total_rows // 4
    copies = []
    for at in (low, low + rows, up, up + rows):
        for source, target in ((orb_hbm, orb_ref), (vel_hbm, vel_ref)):
            part = pl.ds(pl.multiple_of(at, TILE), rows)
            copies.append(pltpu.make_async_copy(source.at[part], target.at[part], sems.at[len(copies)]))
            copies[-1].start()
    ready = 4 if all(which == "near" for which, _, _ in tiles) else 8
    if ready == 8 and all(which == "near" or (which == "far" and j * TILE < rows) for which, _, j in tiles):
        ready = 6
    for copy in copies[:ready]:
        copy.wait()
    product_kernel(orb_ref, vel_ref, away_ref, flip=1, tiles=tiles, side=side, extra=extra)
    for copy in copies[ready:]:
        copy.wait()


def load(orb, vel, tiles):
    whole = jax.ShapeDtypeStruct(orb.shape, orb.dtype)
    return call(
        lambda *refs: load_kernel(*refs, tiles=tiles),
        [jax.ShapeDtypeStruct((len(tiles) * TILE, TILE), BF16), whole, whole],
        12,
        pltpu.with_memory_space_constraint(orb, pltpu.HBM),
        pltpu.with_memory_space_constraint(vel, pltpu.HBM),
        scratch=[pltpu.SemaphoreType.DMA((8,))],
        in_specs=[HBM, HBM],
    )


def halve_kernel(mine_ref, got_ref, send_ref, keep_ref, *, pair):
    rows = send_ref.shape[0]
    bit = side_bit(pair)

    def part(index):
        at = pl.ds(pl.multiple_of(index * rows, PAD), rows)
        return mine_ref[at, :].astype(F32) + got_ref[at, :].astype(F32)

    send_ref[...] = part(1 - bit).astype(BF16)
    keep_ref[...] = part(bit)


def halve(mine, got, pair):
    rows = mine.shape[0] // 2
    out = [jax.ShapeDtypeStruct((rows, TILE), BF16), jax.ShapeDtypeStruct((rows, TILE), F32)]
    return call(lambda *refs: halve_kernel(*refs, pair=pair), out, 2, mine, got)


def add_kernel(a_ref, b_ref, out_ref):
    out_ref[...] = (a_ref[...].astype(F32) + b_ref[...].astype(F32)).astype(BF16)


def add(a, b):
    return call(add_kernel, jax.ShapeDtypeStruct(a.shape, BF16), 2, a, b)


def join_kernel(mine_ref, got_ref, out_ref, *, pair):
    rows = mine_ref.shape[0]
    bit = side_bit(pair)
    out_ref[pl.ds(pl.multiple_of(bit * rows, PAD), rows), :] = mine_ref[...]
    out_ref[pl.ds(pl.multiple_of((1 - bit) * rows, PAD), rows), :] = got_ref[...]


def join(mine, got, pair):
    out = jax.ShapeDtypeStruct((2 * mine.shape[0], TILE), BF16)
    return call(lambda *refs: join_kernel(*refs, pair=pair), out, 2, mine, got)


def share_kernel(a_ref, b_ref, out_ref, *, pairs, diagonal):
    rows = a_ref.shape[0]
    offset = (2 * side_bit(pairs[0]) + side_bit(pairs[1])) * rows
    total = a_ref[...].astype(F32) + b_ref[...].astype(F32)
    out_ref[0:rows, :] = total.astype(BF16)
    square = total * total
    if diagonal:
        tile = (lax.broadcasted_iota(jnp.int32, (rows, TILE), 0) + offset) >> (TILE.bit_length() - 1)
        single = tile == diagonal[0]
        for at in diagonal[1:]:
            single |= tile == at
        square = jnp.where(single, square, 2.0 * square)
    else:
        square = 2.0 * square
    square = jnp.sum(jnp.sum(square, axis=0, keepdims=True), axis=1, keepdims=True)
    high = square.astype(BF16).astype(F32)
    rest = square - high
    middle = rest.astype(BF16).astype(F32)
    small = rest - middle
    line = lax.broadcasted_iota(jnp.int32, (PAD, TILE), 0)
    tail = jnp.where(line == 0, high, jnp.where(line == 1, middle, jnp.where(line == 2, small, 0.0)))
    out_ref[rows : rows + PAD, :] = tail.astype(BF16)


def make_share(a, b, pairs, diagonal):
    out = jax.ShapeDtypeStruct((a.shape[0] + PAD, TILE), BF16)
    return call(lambda *refs: share_kernel(*refs, pairs=pairs, diagonal=diagonal), out, 3, a, b)


def take_tile(ref, index):
    share_rows = ref.shape[0] // SHARES - PAD
    row, end = index * TILE, (index + 1) * TILE
    parts = []
    while row < end:
        share = row // share_rows
        stop = min(end, (share + 1) * share_rows)
        parts.append(ref[row + share * PAD : stop + share * PAD, :])
        row = stop
    return parts[0] if len(parts) == 1 else jnp.concatenate(parts, axis=0)


def tails(refs):
    total = jnp.zeros((1, TILE), F32)
    for ref in refs:
        share = ref.shape[0] // SHARES
        for k in range(SHARES):
            lines = ref[(k + 1) * share - PAD : (k + 1) * share, :].astype(F32)
            total = total + jnp.sum(lines, axis=0, keepdims=True)
    return total


def put_block(ref, i, j, value):
    ref[i * TILE : (i + 1) * TILE, j * TILE : (j + 1) * TILE] = value


def tables(tiles, side):
    result = {"near": {}, "far": {}, "back": {}}
    for n, (which, i, j) in enumerate(tiles):
        if which == "near":
            result["near"][(i, j)] = n
            result["near"][(j, i)] = n
        elif which == "far":
            result["far"][(i, j)] = n
            result["back"][(j, i)] = n
    if any(which == "extra" for which, _, _ in tiles):
        for name in ("far", "back"):
            for i in range(side):
                result[name][(i, i)] = None
    return {name: table for name, table in result.items() if table}


def spans_of(table, side):
    spans = {}
    for p in range(0, side, PANEL):
        columns = [j for (i, j) in table if p <= i < p + PANEL]
        if columns:
            spans[p] = (min(columns), max(columns) + 1)
    return spans


def reach(tiles, flip, side):
    result = set()
    for name, table in tables(tiles, side).items():
        result |= {(1 - flip if name == "back" else flip, p) for p in spans_of(table, side)}
    return result


def fill(piece_ref, tiles, flip, mats, side, extra):
    h, low, up = starts(flip, side)
    found = tables(tiles, side)
    zero = jnp.zeros((TILE, TILE), BF16)
    terms = {}
    for name, table in found.items():
        ref = mats[name]
        for p, (begin, end) in spans_of(table, side).items():
            last = min(p + PANEL, side)
            for i in range(p, last):
                for j in range(begin, end):
                    if table.get((i, j)) is None:
                        put_block(ref, i, j, zero)
            key = (1 - flip if name == "back" else flip, p)
            left = (slice(p * TILE, last * TILE), slice(begin * TILE, end * TILE))
            base = up if name == "far" else low
            terms.setdefault(key, []).append((ref, left, base + begin * TILE, (end - begin) * TILE))
    for n, (which, i, j) in enumerate(tiles):
        value = take_tile(piece_ref, n)
        if which == "near":
            put_block(mats["near"], i, j, value)
            if i != j:
                put_block(mats["near"], j, i, value.T)
        elif which == "far":
            put_block(mats["far"], i, j, value)
            put_block(mats["back"], j, i, value.T)
        else:
            at = pl.ds(pl.multiple_of((h * extra + i) * TILE, TILE), TILE)
            mats["far"][at, at] = value
            mats["back"][at, at] = value.T
    return terms


def apply_kernel(*refs, plan, given, velocities, blocks, final, count, side, extra, names):
    refs = list(refs)
    orb_ref = refs.pop(0)
    vel_ref = refs.pop(0) if velocities else None
    bases = {b: refs.pop(0) for b in given}
    pieces = [refs.pop(0) for _ in plan]
    squares = [refs.pop(0) for _ in range(count)]
    if count:
        refs.pop(0)
    out_hbm = refs.pop(0) if final else None
    norm_hbm = refs.pop(0) if count else None
    outs = {b: refs.pop(0) for b in blocks}
    sems = refs.pop() if final else None
    norm_ref = refs.pop() if count else None
    touched = set().union(*(reach(tiles, flip, side) for tiles, flip in plan))
    copies = []
    _, low, up = starts(0, side)
    base_row = (low, up)

    def rows_of(p):
        return slice(p * TILE, min(p + PANEL, side) * TILE)

    def place(b, p):
        rows = rows_of(p)
        return pl.ds(pl.multiple_of(base_row[b] + rows.start, TILE), rows.stop - rows.start)

    def before(b, p):
        return bases[b][rows_of(p), :] if b in bases else vel_ref[place(b, p), :].astype(F32)

    def send(source, b, p):
        rows = rows_of(p)
        for row in range(rows.start, rows.stop, PIECE):
            at = pl.ds(pl.multiple_of(base_row[b] + row, PIECE), PIECE)
            copy = pltpu.make_async_copy(source.at[row : row + PIECE], out_hbm.at[at], sems.at[len(copies)])
            copy.start()
            copies.append(copy)

    if count:
        square = tails(squares[: count // 2]) + tails(squares[count // 2 :])
        norm_ref[0] = (jnp.sqrt(square) / (2 * side * TILE))[0, 0]
        copies.append(pltpu.make_async_copy(norm_ref, norm_hbm, sems.at[0]))
        copies[0].start()
    for b, p in sorted(final - touched):
        if b in bases:
            send(bases[b], b, p)
        else:
            outs[b][rows_of(p), :] = before(b, p)
            send(outs[b], b, p)
    for b in () if count else blocks:
        for p in range(0, side, PANEL):
            if (b, p) not in touched | final:
                outs[b][rows_of(p), :] = before(b, p)
    terms = {}
    for (tiles, flip), piece, own in zip(plan, pieces, names):
        mats = {name: refs.pop(0) for name in own}
        for key, value in fill(piece, tiles, flip, mats, side, extra).items():
            terms.setdefault(key, []).extend(value)
    for b, p in sorted(touched, key=lambda key: (key not in final, key)):
        total = None
        for ref, left, at, rows in terms[(b, p)]:
            right = orb_ref[pl.ds(pl.multiple_of(at, TILE), rows), :]
            value = jnp.dot(ref[left], right, preferred_element_type=F32)
            total = value if total is None else total + value
        outs[b][rows_of(p), :] = before(b, p) - 0.5 * total
        if (b, p) in final:
            send(outs[b], b, p)
    for copy in copies:
        copy.wait()


def apply(orb, vel, bases, plan, pieces, later=None, squares=(), out=None):
    side, extra = geometry(orb.shape[0])
    wide, columns = side * TILE, orb.shape[1]
    touched = set().union(*(reach(tiles, flip, side) for tiles, flip in plan))
    final = set()
    if later is not None:
        kept = set().union(*(reach(tiles, flip, side) for tiles, flip in later))
        final = {(b, p) for b in (0, 1) for p in range(0, side, PANEL)} - kept
    if squares:
        final = touched
    blocks = [0, 1] if later is not None else sorted({b for b, _ in touched})
    given = [b for b in blocks if bases[b] is not None]
    velocities = len(given) < len(blocks)
    names = [list(tables(tiles, side)) for tiles, _ in plan]
    mats = [pltpu.VMEM((wide, wide), BF16) for own in names for _ in own]
    kernel = lambda *refs: apply_kernel(
        *refs,
        plan=plan,
        given=given,
        velocities=velocities,
        blocks=blocks,
        final=final,
        count=len(squares),
        side=side,
        extra=extra,
        names=names,
    )
    operands = [orb] + ([vel] if velocities else []) + [bases[b] for b in given] + list(pieces) + list(squares)
    block = jax.ShapeDtypeStruct((wide, columns), F32)
    whole = jax.ShapeDtypeStruct(orb.shape, F32)
    sems = [pltpu.SemaphoreType.DMA((len(final) * PANEL * TILE // PIECE + 1,))] if final else []
    mib = 8 + 2 * len(mats)
    if squares:
        return call(
            kernel,
            [whole, jax.ShapeDtypeStruct((1,), F32)],
            mib,
            *operands,
            out,
            scratch=[pltpu.VMEM((wide, columns), F32) for _ in blocks] + mats + [pltpu.SMEM((1,), F32)] + sems,
            in_specs=[VMEM] * len(operands) + [HBM],
            out_specs=[HBM, HBM],
            aliases={len(operands): 0},
        )
    shapes, specs = [block] * len(blocks), [VMEM] * len(blocks)
    if final:
        shapes, specs = [whole] + shapes, [HBM] + specs
    values = list(call(kernel, shapes, mib, *operands, scratch=mats + sems, out_specs=specs))
    out = values.pop(0) if final else None
    result = list(bases)
    for b, value in zip(blocks, values):
        result[b] = value
    return (result, out) if later is not None else result


def permutation(nr, nc, pair):
    result = []
    for r in range(nr):
        for c in range(nc):
            on_r, on_c = pair[(c & 1) ^ parity(r, c)]
            result.append((r * nc + c, (r ^ on_r) * nc + (c ^ on_c ^ parity(on_r, on_c))))
    return result


def routes(nr, nc):
    low = [(1, 0), (0, 2)]
    rest = [(1 << b, 0) for b in range(1, nr.bit_length() - 1)]
    rest += [(0, 1 << b) for b in range(2, nc.bit_length() - 1)]

    def both_ways(bits):
        return list(zip(bits, bits[::-1]))

    usual = (both_ways(low), both_ways(rest))
    result = [usual] * 3
    if len(rest) > 1:
        result[FAR_FIRST] = (both_ways([rest[0], rest[-1]]), both_ways(low + rest[1:-1]))
    return result


def local(orbitals, velocities):
    nr, nc = lax.axis_size("gr"), lax.axis_size("gc")
    chunks = chunk_tiles(orbitals.shape[0])
    plans = routes(nr, nc)
    swap = [(d, d ^ 1) for d in range(nr * nc)]
    joined, far = {}, {}
    for k in TURNS:
        tiles = chunks[k]
        halvings, doublings = plans[k]
        diagonal = [n for n, (which, i, j) in enumerate(tiles) if which == "near" and i == j]

        def move(value, pair):
            return lax.ppermute(value, AXES, swap if pair is None else permutation(nr, nc, pair))

        if k == TURNS[0]:
            send, orbitals, velocities = load(orbitals, velocities, tiles)
        else:
            send = product(1, orbitals, velocities, tiles)
        got = move(send, None)
        mine = product(0, orbitals, velocities, tiles)
        for pair in halvings:
            send, mine = halve(mine, got, pair)
            got = move(send, pair)
        for pair in doublings:
            mine = add(mine, got)
            got = move(mine, pair)
        mine = make_share(mine, got, halvings, diagonal)
        for pair in halvings[::-1]:
            got = move(mine, pair)
            mine = join(mine, got, pair)
        joined[k] = mine
        far[k] = move(mine, None)
    first, second, third = TURNS
    blocks = [None, None]
    blocks = apply(orbitals, velocities, blocks, [(chunks[first], 0)], [joined[first]])
    plan = [(chunks[first], 1)] + [(chunks[second], 0)] * TWO
    blocks = apply(orbitals, velocities, blocks, plan, [far[first]] + [joined[second]] * TWO)
    plan = [(chunks[second], 1), (chunks[third], 0)] + [(chunks[second], 0)] * (1 - TWO)
    pieces = [far[second], joined[third]] + [joined[second]] * (1 - TWO)
    later = [(chunks[third], 1)]
    blocks, out = apply(orbitals, velocities, blocks, plan, pieces, later)
    squares = [joined[k] for k in TURNS] + [far[k] for k in TURNS]
    return tuple(apply(orbitals, velocities, blocks, later, [far[third]], None, squares, out))


def solution(mesh):
    in_specs = (P(None, AXES), P(None, AXES))
    out_specs = (P(None, AXES), P())

    return jax.shard_map(local, mesh=mesh, in_specs=in_specs, out_specs=out_specs, check_vma=False)
```

```python
import jax
import jax.numpy as jnp
from jax import lax
from jax.experimental import pallas as pl
from jax.experimental.pallas import tpu as pltpu
from jax.sharding import PartitionSpec as P


TILE = 128
PAD = 16
SHARES = 4
CUT = 17 / 39
LATE = (1, 2)
TURNS = (0, 1, 2)
FAR_FIRST = 2
TWO = 1
PIECE = 128
PANEL = 1
LOADS = 2
AXES = ("gr", "gc")
BF16 = jnp.bfloat16
F32 = jnp.float32
VMEM = pl.BlockSpec(memory_space=pltpu.VMEM)
SMEM = pl.BlockSpec(memory_space=pltpu.SMEM)
HBM = pl.BlockSpec(memory_space=pltpu.HBM)
DIMS = (((1,), (1,)), ((), ()))


def params(mib):
    return pltpu.CompilerParams(vmem_limit_bytes=mib * 2**20)


def call(kernel, out, mib, *operands, scratch=(), in_specs=None, out_specs=None, aliases={}):
    return pl.pallas_call(
        kernel,
        out_shape=out,
        in_specs=in_specs or [VMEM] * len(operands),
        out_specs=out_specs or jax.tree.map(lambda _: VMEM, out),
        scratch_shapes=scratch,
        input_output_aliases=aliases,
        compiler_params=params(mib),
    )(*operands)


def geometry(total_rows):
    side = total_rows // TILE // 2
    return side, side // 2


def chunk_tiles(total_rows):
    side, extra = geometry(total_rows)
    near = [("near", i, j) for j in range(side) for i in range(j + 1)]
    far = [("far", i, j) for j in range(side) for i in range(j + 1, side)]
    late = [at for at in near if at[1] >= side - LATE[0] and at[2] == side - 1] + [at for at in far if at[2] >= LATE[1]]
    tiles = [at for at in near if at not in late]
    tiles += [("extra", k, k) for k in range(extra)]
    tiles += [at for at in far if at not in late]
    cut = round(CUT * (len(tiles) + len(late)))
    return [tiles[:cut], tiles[cut:], late]


def parity(r, c):
    return (r ^ (r >> 1) ^ (c >> 1)) & 1


def pick(half, pair):
    return tuple(jnp.where(half == 0, a, b) for a, b in zip(*pair))


def position():
    r, c = lax.axis_index("gr"), lax.axis_index("gc")
    return r, c, (c & 1) ^ parity(r, c)


def side_bit(pair):
    r, c, half = position()
    on_r, on_c = pick(half, pair)
    return (((r & on_r) | (c & on_c)) != 0).astype(jnp.int32)


def starts(flip, side):
    _, _, half = position()
    h = half ^ flip
    low = pl.multiple_of(h * (side * TILE), TILE)
    up = pl.multiple_of((1 - h) * (side * TILE), TILE)
    return h, low, up


def symmetric(orb_ref, vel_ref, r0, rows, c0, cols):
    one = lax.dot_general(
        orb_ref[pl.ds(r0, rows), :], vel_ref[pl.ds(c0, cols), :], DIMS, preferred_element_type=F32
    )
    two = lax.dot_general(
        vel_ref[pl.ds(r0, rows), :], orb_ref[pl.ds(c0, cols), :], DIMS, preferred_element_type=F32
    )
    return one + two


def product_kernel(orb_ref, vel_ref, out_ref, *, flip, tiles, side, extra):
    h, low, up = starts(flip, side)
    for kind in ("near", "far"):
        table = {(i, j): n for n, (which, i, j) in enumerate(tiles) if which == kind}
        for c in range(0, side, 2):
            columns = [j for j in (c, c + 1) if any(at[1] == j for at in table)]
            if not columns:
                continue
            rows = [i for i in range(side) if any((i, j) in table for j in columns)]
            rows = list(range(rows[0], rows[-1] + 1))
            value = symmetric(
                orb_ref,
                vel_ref,
                low + rows[0] * TILE,
                len(rows) * TILE,
                (low if kind == "near" else up) + columns[0] * TILE,
                len(columns) * TILE,
            )
            for i in rows:
                for j in columns:
                    if (i, j) in table:
                        at = table[(i, j)] * TILE
                        row, col = (i - rows[0]) * TILE, (j - columns[0]) * TILE
                        out_ref[at : at + TILE, :] = value[row : row + TILE, col : col + TILE].astype(BF16)
    for n, (which, k, _) in enumerate(tiles):
        if which == "extra":
            shift = pl.multiple_of((h * extra + k) * TILE, TILE)
            value = symmetric(orb_ref, vel_ref, low + shift, TILE, up + shift, TILE)
            out_ref[n * TILE : (n + 1) * TILE, :] = value.astype(BF16)


def product(flip, orb, vel, tiles):
    side, extra = geometry(orb.shape[0])
    kernel = lambda *refs: product_kernel(*refs, flip=flip, tiles=tiles, side=side, extra=extra)
    return call(kernel, jax.ShapeDtypeStruct((len(tiles) * TILE, TILE), BF16), 6, orb, vel)


def load_kernel(orb_hbm, vel_hbm, away_ref, orb_ref, vel_ref, sems, *, tiles):
    total_rows = orb_hbm.shape[0]
    side, extra = geometry(total_rows)
    _, low, up = starts(1, side)
    half = side * TILE
    copies = []

    def start(begin, parts):
        for at in range(0, half, half // parts):
            for source, target in ((orb_hbm, orb_ref), (vel_hbm, vel_ref)):
                part = pl.ds(pl.multiple_of(begin + at, TILE), half // parts)
                copies.append(pltpu.make_async_copy(source.at[part], target.at[part], sems.at[len(copies)]))
                copies[-1].start()

    start(low, LOADS)
    start(up, LOADS)
    ready = 2 * LOADS if all(which == "near" for which, _, _ in tiles) else 4 * LOADS
    for copy in copies[:ready]:
        copy.wait()
    product_kernel(orb_ref, vel_ref, away_ref, flip=1, tiles=tiles, side=side, extra=extra)
    for copy in copies[ready:]:
        copy.wait()


def load(orb, vel, tiles):
    whole = jax.ShapeDtypeStruct(orb.shape, orb.dtype)
    return call(
        lambda *refs: load_kernel(*refs, tiles=tiles),
        [jax.ShapeDtypeStruct((len(tiles) * TILE, TILE), BF16), whole, whole],
        12,
        pltpu.with_memory_space_constraint(orb, pltpu.HBM),
        pltpu.with_memory_space_constraint(vel, pltpu.HBM),
        scratch=[pltpu.SemaphoreType.DMA((4 * LOADS,))],
        in_specs=[HBM, HBM],
    )


def halve_kernel(mine_ref, got_ref, send_ref, keep_ref, *, pair):
    rows = send_ref.shape[0]
    bit = side_bit(pair)

    def part(index):
        at = pl.ds(pl.multiple_of(index * rows, PAD), rows)
        return mine_ref[at, :].astype(F32) + got_ref[at, :].astype(F32)

    send_ref[...] = part(1 - bit).astype(BF16)
    keep_ref[...] = part(bit)


def halve(mine, got, pair):
    rows = mine.shape[0] // 2
    out = [jax.ShapeDtypeStruct((rows, TILE), BF16), jax.ShapeDtypeStruct((rows, TILE), F32)]
    return call(lambda *refs: halve_kernel(*refs, pair=pair), out, 2, mine, got)


def add_kernel(a_ref, b_ref, out_ref):
    out_ref[...] = (a_ref[...].astype(F32) + b_ref[...].astype(F32)).astype(BF16)


def add(a, b):
    return call(add_kernel, jax.ShapeDtypeStruct(a.shape, BF16), 2, a, b)


def join_kernel(mine_ref, got_ref, out_ref, *, pair):
    rows = mine_ref.shape[0]
    bit = side_bit(pair)
    out_ref[pl.ds(pl.multiple_of(bit * rows, PAD), rows), :] = mine_ref[...]
    out_ref[pl.ds(pl.multiple_of((1 - bit) * rows, PAD), rows), :] = got_ref[...]


def join(mine, got, pair):
    out = jax.ShapeDtypeStruct((2 * mine.shape[0], TILE), BF16)
    return call(lambda *refs: join_kernel(*refs, pair=pair), out, 2, mine, got)


def share_kernel(a_ref, b_ref, out_ref, *, pairs, diagonal):
    rows = a_ref.shape[0]
    offset = (2 * side_bit(pairs[0]) + side_bit(pairs[1])) * rows
    total = a_ref[...].astype(F32) + b_ref[...].astype(F32)
    out_ref[0:rows, :] = total.astype(BF16)
    square = total * total
    if diagonal:
        tile = (lax.broadcasted_iota(jnp.int32, (rows, TILE), 0) + offset) >> (TILE.bit_length() - 1)
        single = tile == diagonal[0]
        for at in diagonal[1:]:
            single |= tile == at
        square = jnp.where(single, square, 2.0 * square)
    else:
        square = 2.0 * square
    square = jnp.sum(jnp.sum(square, axis=0, keepdims=True), axis=1, keepdims=True)
    high = square.astype(BF16).astype(F32)
    rest = square - high
    middle = rest.astype(BF16).astype(F32)
    small = rest - middle
    line = lax.broadcasted_iota(jnp.int32, (PAD, TILE), 0)
    tail = jnp.where(line == 0, high, jnp.where(line == 1, middle, jnp.where(line == 2, small, 0.0)))
    out_ref[rows : rows + PAD, :] = tail.astype(BF16)


def make_share(a, b, pairs, diagonal):
    out = jax.ShapeDtypeStruct((a.shape[0] + PAD, TILE), BF16)
    return call(lambda *refs: share_kernel(*refs, pairs=pairs, diagonal=diagonal), out, 3, a, b)


def take_tile(ref, index):
    share_rows = ref.shape[0] // SHARES - PAD
    row, end = index * TILE, (index + 1) * TILE
    parts = []
    while row < end:
        share = row // share_rows
        stop = min(end, (share + 1) * share_rows)
        parts.append(ref[row + share * PAD : stop + share * PAD, :])
        row = stop
    return parts[0] if len(parts) == 1 else jnp.concatenate(parts, axis=0)


def tails(refs):
    total = jnp.zeros((1, TILE), F32)
    for ref in refs:
        share = ref.shape[0] // SHARES
        for k in range(SHARES):
            lines = ref[(k + 1) * share - PAD : (k + 1) * share, :].astype(F32)
            total = total + jnp.sum(lines, axis=0, keepdims=True)
    return total


def put_block(ref, i, j, value):
    ref[i * TILE : (i + 1) * TILE, j * TILE : (j + 1) * TILE] = value


def tables(tiles, side):
    result = {"near": {}, "far": {}, "back": {}}
    for n, (which, i, j) in enumerate(tiles):
        if which == "near":
            result["near"][(i, j)] = n
            result["near"][(j, i)] = n
        elif which == "far":
            result["far"][(i, j)] = n
            result["back"][(j, i)] = n
    if any(which == "extra" for which, _, _ in tiles):
        for name in ("far", "back"):
            for i in range(side):
                result[name][(i, i)] = None
    return {name: table for name, table in result.items() if table}


def spans_of(table, side):
    spans = {}
    for p in range(0, side, PANEL):
        columns = [j for (i, j) in table if p <= i < p + PANEL]
        if columns:
            spans[p] = (min(columns), max(columns) + 1)
    return spans


def reach(tiles, flip, side):
    result = set()
    for name, table in tables(tiles, side).items():
        result |= {(1 - flip if name == "back" else flip, p) for p in spans_of(table, side)}
    return result


def fill(piece_ref, tiles, flip, mats, side, extra):
    h, low, up = starts(flip, side)
    found = tables(tiles, side)
    zero = jnp.zeros((TILE, TILE), BF16)
    terms = {}
    for name, table in found.items():
        ref = mats[name]
        for p, (begin, end) in spans_of(table, side).items():
            last = min(p + PANEL, side)
            for i in range(p, last):
                for j in range(begin, end):
                    if table.get((i, j)) is None:
                        put_block(ref, i, j, zero)
            key = (1 - flip if name == "back" else flip, p)
            left = (slice(p * TILE, last * TILE), slice(begin * TILE, end * TILE))
            base = up if name == "far" else low
            terms.setdefault(key, []).append((ref, left, base + begin * TILE, (end - begin) * TILE))
    for n, (which, i, j) in enumerate(tiles):
        value = take_tile(piece_ref, n)
        if which == "near":
            put_block(mats["near"], i, j, value)
            if i != j:
                put_block(mats["near"], j, i, value.T)
        elif which == "far":
            put_block(mats["far"], i, j, value)
            put_block(mats["back"], j, i, value.T)
        else:
            at = pl.ds(pl.multiple_of((h * extra + i) * TILE, TILE), TILE)
            mats["far"][at, at] = value
            mats["back"][at, at] = value.T
    return terms


def apply_kernel(*refs, plan, given, velocities, blocks, final, count, side, extra, names):
    refs = list(refs)
    orb_ref = refs.pop(0)
    vel_ref = refs.pop(0) if velocities else None
    bases = {b: refs.pop(0) for b in given}
    pieces = [refs.pop(0) for _ in plan]
    squares = [refs.pop(0) for _ in range(count)]
    if count:
        refs.pop(0)
    out_hbm = refs.pop(0) if final else None
    norm_hbm = refs.pop(0) if count else None
    outs = {b: refs.pop(0) for b in blocks}
    sems = refs.pop() if final else None
    norm_ref = refs.pop() if count else None
    touched = set().union(*(reach(tiles, flip, side) for tiles, flip in plan))
    copies = []
    _, low, up = starts(0, side)
    base_row = (low, up)

    def rows_of(p):
        return slice(p * TILE, min(p + PANEL, side) * TILE)

    def place(b, p):
        rows = rows_of(p)
        return pl.ds(pl.multiple_of(base_row[b] + rows.start, TILE), rows.stop - rows.start)

    def before(b, p):
        return bases[b][rows_of(p), :] if b in bases else vel_ref[place(b, p), :].astype(F32)

    def send(source, b, p):
        rows = rows_of(p)
        for row in range(rows.start, rows.stop, PIECE):
            at = pl.ds(pl.multiple_of(base_row[b] + row, PIECE), PIECE)
            copy = pltpu.make_async_copy(source.at[row : row + PIECE], out_hbm.at[at], sems.at[len(copies)])
            copy.start()
            copies.append(copy)

    if count:
        square = tails(squares[: count // 2]) + tails(squares[count // 2 :])
        norm_ref[0] = (jnp.sqrt(square) / (2 * side * TILE))[0, 0]
        copies.append(pltpu.make_async_copy(norm_ref, norm_hbm, sems.at[0]))
        copies[0].start()
    for b, p in sorted(final - touched):
        if b in bases:
            send(bases[b], b, p)
        else:
            outs[b][rows_of(p), :] = before(b, p)
            send(outs[b], b, p)
    for b in () if count else blocks:
        for p in range(0, side, PANEL):
            if (b, p) not in touched | final:
                outs[b][rows_of(p), :] = before(b, p)
    terms = {}
    for (tiles, flip), piece, own in zip(plan, pieces, names):
        mats = {name: refs.pop(0) for name in own}
        for key, value in fill(piece, tiles, flip, mats, side, extra).items():
            terms.setdefault(key, []).extend(value)
    for b, p in sorted(touched, key=lambda key: (key not in final, key)):
        total = None
        for ref, left, at, rows in terms[(b, p)]:
            right = orb_ref[pl.ds(pl.multiple_of(at, TILE), rows), :]
            value = jnp.dot(ref[left], right, preferred_element_type=F32)
            total = value if total is None else total + value
        outs[b][rows_of(p), :] = before(b, p) - 0.5 * total
        if (b, p) in final:
            send(outs[b], b, p)
    for copy in copies:
        copy.wait()


def apply(orb, vel, bases, plan, pieces, later=None, squares=(), out=None):
    side, extra = geometry(orb.shape[0])
    wide, columns = side * TILE, orb.shape[1]
    touched = set().union(*(reach(tiles, flip, side) for tiles, flip in plan))
    final = set()
    if later is not None:
        kept = set().union(*(reach(tiles, flip, side) for tiles, flip in later))
        final = {(b, p) for b in (0, 1) for p in range(0, side, PANEL)} - kept
    if squares:
        final = touched
    blocks = [0, 1] if later is not None else sorted({b for b, _ in touched})
    given = [b for b in blocks if bases[b] is not None]
    velocities = len(given) < len(blocks)
    names = [list(tables(tiles, side)) for tiles, _ in plan]
    mats = [pltpu.VMEM((wide, wide), BF16) for own in names for _ in own]
    kernel = lambda *refs: apply_kernel(
        *refs,
        plan=plan,
        given=given,
        velocities=velocities,
        blocks=blocks,
        final=final,
        count=len(squares),
        side=side,
        extra=extra,
        names=names,
    )
    operands = [orb] + ([vel] if velocities else []) + [bases[b] for b in given] + list(pieces) + list(squares)
    block = jax.ShapeDtypeStruct((wide, columns), F32)
    whole = jax.ShapeDtypeStruct(orb.shape, F32)
    sems = [pltpu.SemaphoreType.DMA((len(final) * PANEL * TILE // PIECE + 1,))] if final else []
    mib = 8 + 2 * len(mats)
    if squares:
        return call(
            kernel,
            [whole, jax.ShapeDtypeStruct((1,), F32)],
            mib,
            *operands,
            out,
            scratch=[pltpu.VMEM((wide, columns), F32) for _ in blocks] + mats + [pltpu.SMEM((1,), F32)] + sems,
            in_specs=[VMEM] * len(operands) + [HBM],
            out_specs=[HBM, HBM],
            aliases={len(operands): 0},
        )
    shapes, specs = [block] * len(blocks), [VMEM] * len(blocks)
    if final:
        shapes, specs = [whole] + shapes, [HBM] + specs
    values = list(call(kernel, shapes, mib, *operands, scratch=mats + sems, out_specs=specs))
    out = values.pop(0) if final else None
    result = list(bases)
    for b, value in zip(blocks, values):
        result[b] = value
    return (result, out) if later is not None else result


def permutation(nr, nc, pair):
    result = []
    for r in range(nr):
        for c in range(nc):
            on_r, on_c = pair[(c & 1) ^ parity(r, c)]
            result.append((r * nc + c, (r ^ on_r) * nc + (c ^ on_c ^ parity(on_r, on_c))))
    return result


def routes(nr, nc):
    low = [(1, 0), (0, 2)]
    rest = [(1 << b, 0) for b in range(1, nr.bit_length() - 1)]
    rest += [(0, 1 << b) for b in range(2, nc.bit_length() - 1)]

    def both_ways(bits):
        return list(zip(bits, bits[::-1]))

    usual = (both_ways(low), both_ways(rest))
    result = [usual] * 3
    if len(rest) > 1:
        result[FAR_FIRST] = (both_ways([rest[0], rest[-1]]), both_ways(low + rest[1:-1]))
    return result


def local(orbitals, velocities):
    nr, nc = lax.axis_size("gr"), lax.axis_size("gc")
    chunks = chunk_tiles(orbitals.shape[0])
    plans = routes(nr, nc)
    swap = [(d, d ^ 1) for d in range(nr * nc)]
    joined, far = {}, {}
    for k in TURNS:
        tiles = chunks[k]
        halvings, doublings = plans[k]
        diagonal = [n for n, (which, i, j) in enumerate(tiles) if which == "near" and i == j]

        def move(value, pair):
            return lax.ppermute(value, AXES, swap if pair is None else permutation(nr, nc, pair))

        if k == TURNS[0]:
            send, orbitals, velocities = load(orbitals, velocities, tiles)
        else:
            send = product(1, orbitals, velocities, tiles)
        got = move(send, None)
        mine = product(0, orbitals, velocities, tiles)
        for pair in halvings:
            send, mine = halve(mine, got, pair)
            got = move(send, pair)
        for pair in doublings:
            mine = add(mine, got)
            got = move(mine, pair)
        mine = make_share(mine, got, halvings, diagonal)
        for pair in halvings[::-1]:
            got = move(mine, pair)
            mine = join(mine, got, pair)
        joined[k] = mine
        far[k] = move(mine, None)
    first, second, third = TURNS
    blocks = [None, None]
    blocks = apply(orbitals, velocities, blocks, [(chunks[first], 0)], [joined[first]])
    plan = [(chunks[first], 1)] + [(chunks[second], 0)] * TWO
    blocks = apply(orbitals, velocities, blocks, plan, [far[first]] + [joined[second]] * TWO)
    plan = [(chunks[second], 1), (chunks[third], 0)] + [(chunks[second], 0)] * (1 - TWO)
    pieces = [far[second], joined[third]] + [joined[second]] * (1 - TWO)
    later = [(chunks[third], 1)]
    blocks, out = apply(orbitals, velocities, blocks, plan, pieces, later)
    squares = [joined[k] for k in TURNS] + [far[k] for k in TURNS]
    return tuple(apply(orbitals, velocities, blocks, later, [far[third]], None, squares, out))


def solution(mesh):
    in_specs = (P(None, AXES), P(None, AXES))
    out_specs = (P(None, AXES), P())

    return jax.shard_map(local, mesh=mesh, in_specs=in_specs, out_specs=out_specs, check_vma=False)
```
